32 devices in a mesh: dp: 1 (over z), cpo: 4 (over y), cpi: 8 (over x, core).
Axes of the slice: x: 4, y: 4, z: 1, core: 2. Of those that a mesh axis runs over, the one named last changes fastest.
The devices are a block of a 4x4x8 slice.
Arguments:
- hidden: bfloat16 [8192, 4096], P(('dp', 'cpo', 'cpi'))
- w_query: bfloat16 [4096, 32, 128], replicated
- w_key: bfloat16 [4096, 32, 128], replicated
- w_value: bfloat16 [4096, 32, 128], replicated
- w_out: bfloat16 [32, 128, 4096], replicated
Outputs:
- output: bfloat16 [8192, 4096], P(('dp', 'cpo', 'cpi'))
All inputs are finite; a program needn't handle non-finite values.
Results may differ from the reference program's by a relative error of at most 0.00592155.
Values are sent between devices in bfloat16 or wider.
A program may use at most 768 MiB of HBM per device.

```python
import jax
import jax.numpy as jnp
from jax import lax

MODEL_DIM = 4096
Q_HEADS = 32
KV_HEADS = 32
HEAD_DIM = 128
TOK_DEV = 256
OUTER_DEVS = 4
INNER_DEVS = 8
ROPE_BASE = 500000.0


def token_positions():
    n_dev = OUTER_DEVS * INNER_DEVS
    chunk_len = TOK_DEV // 2
    row_ids = jnp.arange(n_dev * TOK_DEV, dtype=jnp.int32)
    owner_dev = row_ids // TOK_DEV
    second_half = (row_ids // chunk_len) % 2
    chunk_idx = jnp.where(second_half == 0, owner_dev, 2 * n_dev - 1 - owner_dev)
    return chunk_idx * chunk_len + row_ids % chunk_len


def rope_tables(positions):
    half_dim = HEAD_DIM // 2
    inv_freq = ROPE_BASE ** (-(2.0 / HEAD_DIM) * jnp.arange(half_dim, dtype=jnp.float32))
    angles = positions.astype(jnp.float32)[:, None] * inv_freq[None, :]
    return jnp.cos(angles), jnp.sin(angles)


def apply_rope(proj_in, cos_b, sin_b):
    half_dim = proj_in.shape[-1] // 2
    lower_half = proj_in[..., :half_dim]
    upper_half = proj_in[..., half_dim:]
    return jnp.concatenate([lower_half * cos_b - upper_half * sin_b, upper_half * cos_b + lower_half * sin_b], axis=-1)


def setup_inputs(seed: int = 0, part: int = 0) -> dict:
    n_dev = OUTER_DEVS * INNER_DEVS
    seq_len = n_dev * TOK_DEV
    chunk_len = TOK_DEV // 2
    root_key = jax.random.key(seed)
    part_root, shared_root = jax.random.split(root_key)
    part_key = jax.random.fold_in(part_root, part)
    noise_key, chunk_key = jax.random.split(part_key)
    wq_key, wk_key, wv_key, wo_key = jax.random.split(shared_root, 4)
    chunk_means = jax.random.normal(chunk_key, (2 * n_dev, MODEL_DIM), jnp.float32)
    chunk_of_row = token_positions() // chunk_len
    noise_rows = jax.random.normal(noise_key, (seq_len, MODEL_DIM), jnp.float32)
    hidden = 0.6 * noise_rows + chunk_means[chunk_of_row]
    in_scale = MODEL_DIM ** -0.5
    out_scale = (Q_HEADS * HEAD_DIM) ** -0.5
    w_query = jax.random.normal(wq_key, (MODEL_DIM, Q_HEADS, HEAD_DIM), jnp.float32) * in_scale
    w_key = jax.random.normal(wk_key, (MODEL_DIM, KV_HEADS, HEAD_DIM), jnp.float32) * in_scale
    w_value = jax.random.normal(wv_key, (MODEL_DIM, KV_HEADS, HEAD_DIM), jnp.float32) * in_scale
    w_out = jax.random.normal(wo_key, (Q_HEADS, HEAD_DIM, MODEL_DIM), jnp.float32) * out_scale
    return dict(hidden=hidden.astype(jnp.bfloat16), w_query=w_query.astype(jnp.bfloat16), w_key=w_key.astype(jnp.bfloat16), w_value=w_value.astype(jnp.bfloat16), w_out=w_out.astype(jnp.bfloat16))


def reference(hidden, w_query, w_key, w_value, w_out):
    n_dev = OUTER_DEVS * INNER_DEVS
    seq_len = n_dev * TOK_DEV
    n_chunks = 2 * n_dev
    chunk_len = TOK_DEV // 2
    group_size = Q_HEADS // KV_HEADS
    score_scale = HEAD_DIM ** -0.5
    positions = token_positions()
    cos_t, sin_t = rope_tables(positions)
    cos_b = cos_t[:, None, :]
    sin_b = sin_t[:, None, :]
    q_proj = jnp.dot(hidden, w_query.reshape(MODEL_DIM, Q_HEADS * HEAD_DIM), preferred_element_type=jnp.float32)
    k_proj = jnp.dot(hidden, w_key.reshape(MODEL_DIM, KV_HEADS * HEAD_DIM), preferred_element_type=jnp.float32)
    v_proj = jnp.dot(hidden, w_value.reshape(MODEL_DIM, KV_HEADS * HEAD_DIM), preferred_element_type=jnp.float32)
    queries = apply_rope(q_proj.reshape(seq_len, Q_HEADS, HEAD_DIM), cos_b, sin_b).astype(jnp.bfloat16)
    keys_rot = apply_rope(k_proj.reshape(seq_len, KV_HEADS, HEAD_DIM), cos_b, sin_b).astype(jnp.bfloat16)
    values_bf = v_proj.reshape(seq_len, KV_HEADS, HEAD_DIM).astype(jnp.bfloat16)
    q_heads = queries.astype(jnp.float32).reshape(n_chunks, chunk_len, KV_HEADS, group_size, HEAD_DIM).transpose(2, 0, 3, 1, 4)
    k_heads = keys_rot.astype(jnp.float32).transpose(1, 0, 2)
    v_heads = values_bf.astype(jnp.float32).transpose(1, 0, 2)
    q_pos = positions.reshape(n_chunks, chunk_len)

    def one_head(head_args):
        q_head, k_head, v_head = head_args

        def one_chunk(chunk_args):
            q_chunk, pos_chunk = chunk_args
            scores = jnp.einsum('gqd,sd->gqs', q_chunk, k_head) * score_scale
            causal = positions[None, None, :] <= pos_chunk[None, :, None]
            scores = jnp.where(causal, scores, -jnp.inf)
            probs_blk = jax.nn.softmax(scores, axis=-1)
            return jnp.einsum('gqs,sd->gqd', probs_blk, v_head)

        return lax.map(one_chunk, (q_head, q_pos))

    attn_rows = lax.map(one_head, (q_heads, k_heads, v_heads))
    attn_rows = attn_rows.transpose(1, 3, 0, 2, 4).reshape(seq_len, Q_HEADS * HEAD_DIM).astype(jnp.bfloat16)
    out_rows = jnp.dot(attn_rows, w_out.reshape(Q_HEADS * HEAD_DIM, MODEL_DIM), preferred_element_type=jnp.float32)
    return out_rows.astype(jnp.bfloat16)
```

```python
import functools
import math

import jax
import jax.numpy as jnp
from jax import lax
from jax.experimental import pallas as pl
from jax.experimental.pallas import tpu as pltpu
from jax.sharding import PartitionSpec as P

ROPE_BASE = 500000.0
NEG_BIG = -1e30
MESH = pl.DeviceIdType.MESH
PIECES = 8
F32 = jnp.float32
BF16 = jnp.bfloat16


def remote(src, dst, send_sem, recv_sem, y, i):
    return pltpu.make_async_remote_copy(src_ref=src, dst_ref=dst, send_sem=send_sem, recv_sem=recv_sem, device_id={'cpo': y, 'cpi': i}, device_id_type=MESH)


def wait_bytes(ref, sem):
    pltpu.make_async_copy(ref, ref, sem).wait()


def piece_half(p):
    return jnp.where(p < 2, p, jnp.where(p < 4, 0, jnp.where(p < 6, 1, p - 6)))


def piece_dy(p, n_outer):
    return jnp.where(p < 2, 0, jnp.where(p < 6, jnp.where(lax.rem(p, 2) == 0, n_outer - 1, 1), 2))


def qkv_kernel(n_outer, n_inner, hid_in, wq, wk, wv, cos_ref, sin_ref, qkv_out,
               hid_buf, raw, wide, wbuf, stage, relay,
               h_send, h_recv, h_load, w_sem, s_send, l_sem, r_send, r_recv, q_recv):
    y = lax.axis_index('cpo')
    i = lax.axis_index('cpi')
    n_x = n_inner // 2
    x = i // 2
    c = lax.rem(i, 2)
    chunk = hid_buf.shape[1]
    n_chunks = qkv_out.shape[0]
    depth = raw.shape[1]
    n_k = wbuf.shape[1] // depth
    y_up = lax.rem(y + 1, n_outer)
    y_dn = lax.rem(y + n_outer - 1, n_outer)
    x_up = lax.rem(x + 1, n_x)
    x_dn = lax.rem(x + n_x - 1, n_x)
    weights = (wq, wk, wv)
    n_raw = raw.shape[0]

    def w_copy(t, kc, slot):
        src = weights[t].at[pl.ds(kc * depth, depth), pl.ds(pl.multiple_of(y * n_inner, n_inner), n_inner)]
        return pltpu.make_async_copy(src, raw.at[slot], w_sem.at[slot])

    for slot in range(n_raw):
        w_copy(0, slot, slot).start()
    own = [pltpu.make_async_copy(hid_in.at[pl.ds(f * chunk, chunk)], hid_buf.at[f], h_load.at[f]) for f in range(2)]
    for cp in own:
        cp.start()

    barrier = pltpu.get_barrier_semaphore()
    pl.semaphore_signal(barrier, inc=1, device_id={'cpo': y_up, 'cpi': i}, device_id_type=MESH)
    pl.semaphore_signal(barrier, inc=1, device_id={'cpo': y_dn, 'cpi': i}, device_id_type=MESH)
    for d in range(1, n_inner):
        pl.semaphore_signal(barrier, inc=1, device_id={'cpo': y, 'cpi': lax.rem(i + d, n_inner)}, device_id_type=MESH)
    pl.semaphore_wait(barrier, n_inner + 1)

    hid_sends = []
    for f in range(2):
        src = hid_in.at[pl.ds(f * chunk, chunk)]
        hid_sends.append(remote(src, hid_buf.at[2 + 2 * f], h_send.at[2 * f], h_recv.at[2 + 2 * f], y_up, i))
        hid_sends.append(remote(src, hid_buf.at[3 + 2 * f], h_send.at[2 * f + 1], h_recv.at[3 + 2 * f], y_dn, i))
    for cp in hid_sends:
        cp.start()
    fwd_up = remote(hid_buf.at[2], hid_buf.at[6], h_send.at[4], h_recv.at[6], y_up, i)
    fwd_dn = remote(hid_buf.at[5], hid_buf.at[7], h_send.at[5], h_recv.at[7], y_dn, i)

    for t in range(3):
        def relayout(kc, _, t=t):
            slot = lax.rem(t * n_k + kc, n_raw)
            w_copy(t, kc, slot).wait()
            wide[...] = raw[slot].astype(F32)
            for j in range(n_inner):
                col = (j % 2) * 384 + t * 128
                wbuf[j // 2, pl.ds(pl.multiple_of(kc * depth, depth), depth), col:col + 128] = wide[:, j, :].astype(BF16)
            nxt = kc + n_raw

            @pl.when(nxt < n_k)
            def _():
                w_copy(t, nxt, slot).start()

            if t < 2:
                @pl.when(nxt >= n_k)
                def _():
                    w_copy(t + 1, nxt - n_k, slot).start()
            return 0

        lax.fori_loop(0, n_k, relayout, 0)
    for cp in own:
        cp.wait()

    def chunk_index(p, src_i):
        rank = lax.rem(y + piece_dy(p, n_outer), n_outer) * n_inner + src_i
        return jnp.where(piece_half(p) == 0, rank, n_chunks - 1 - rank)

    def relay_copy(p, c2):
        front = piece_half(p) == 0
        src_x = jnp.where(front, x_dn, x_up)
        dst_x = jnp.where(front, x_up, x_dn)
        return remote(relay.at[p, c2], qkv_out.at[chunk_index(p, src_x * 2 + c)], r_send, q_recv, y, dst_x * 2 + c2)

    def forward_relay(p):
        for c2 in range(2):
            wait_bytes_remote = pltpu.make_async_copy(relay.at[p, c2], relay.at[p, c2], r_recv.at[p, c2])
            wait_bytes_remote.wait()
            relay_copy(p, c2).start()

    def piece(p, _):
        @pl.when(jnp.logical_and(p >= 2, p != 5))
        def _():
            wait_bytes(hid_buf.at[p], h_recv.at[p])

        @pl.when(p == 2)
        def _():
            fwd_up.start()

        @pl.when(p == 4)
        def _():
            wait_bytes(hid_buf.at[5], h_recv.at[5])
            fwd_dn.start()

        cos_p = cos_ref[p]
        sin_p = sin_ref[p]

        def rope(a):
            return a * cos_p + pltpu.roll(a, 64, 1) * sin_p

        out_t = chunk_index(p, i)

        def per_chip(kk, _):
            xc = lax.rem(x + jnp.where(kk == 0, 2, jnp.where(kk == 1, 1, jnp.where(kk == 2, n_x - 1, 0))), n_x)
            acc = jnp.dot(hid_buf[p], wbuf[xc], preferred_element_type=F32)
            for c2 in range(2):
                col = c2 * 384
                stage[p, xc * 2 + c2, 0] = rope(acc[:, col:col + 128]).astype(BF16)
                stage[p, xc * 2 + c2, 1] = rope(acc[:, col + 128:col + 256]).astype(BF16)
                stage[p, xc * 2 + c2, 2] = acc[:, col + 256:col + 384].T.astype(BF16)

            @pl.when(kk == 0)
            def _():
                via = jnp.where(piece_half(p) == 0, x_up, x_dn)
                for c2 in range(2):
                    remote(stage.at[p, xc * 2 + c2], relay.at[p, c2], s_send, r_recv.at[p, c2], y, via * 2 + c).start()

            @pl.when(jnp.logical_and(kk >= 1, kk <= 2))
            def _():
                for c2 in range(2):
                    remote(stage.at[p, xc * 2 + c2], qkv_out.at[out_t], s_send, q_recv, y, xc * 2 + c2).start()

            @pl.when(kk == 3)
            def _():
                remote(stage.at[p, xc * 2 + 1 - c], qkv_out.at[out_t], s_send, q_recv, y, xc * 2 + 1 - c).start()
                pltpu.make_async_copy(stage.at[p, i], qkv_out.at[out_t], l_sem).start()
            return 0

        lax.fori_loop(0, n_x, per_chip, 0)

        @pl.when(p >= 1)
        def _():
            forward_relay(p - 1)
        return 0

    lax.fori_loop(0, PIECES, piece, 0)
    forward_relay(PIECES - 1)

    for cp in hid_sends:
        cp.wait_send()
    fwd_up.wait_send()
    fwd_dn.wait_send()
    wait_bytes(stage.at[:, pl.ds(0, n_inner - 1)], s_send)
    wait_bytes(relay, r_send)
    wait_bytes(qkv_out.at[pl.ds(0, PIECES)], l_sem)
    wait_bytes(qkv_out.at[pl.ds(0, n_chunks - PIECES)], q_recv)


def attn_kernel(n_outer, n_inner, score_scale, qkv_hbm, wout_hbm, out_ref,
                qkv, wbuf, s0, s1, m_ref, l_ref, acc_ref, o_stage, o_recv, ld_sem, w_sem, o_send, o_sem):
    y = lax.axis_index('cpo')
    i = lax.axis_index('cpi')
    me = y * n_inner + i
    n_dev = n_outer * n_inner
    head_dim = qkv.shape[2]
    chunk = qkv.shape[3]
    tk, tq = s0.shape
    kc = tk // chunk
    qc = tq // chunk
    n_q = qkv.shape[0] // qc
    strip = 256
    n_strips = tq // strip
    n_w = wbuf.shape[0]
    wide = wbuf.shape[2]
    c_exp = score_scale * math.log2(math.e)

    load = pltpu.make_async_copy(qkv_hbm, qkv, ld_sem)
    load.start()

    barrier = pltpu.get_barrier_semaphore()

    def sig(d, _):
        peer = lax.rem(me + d, n_dev)
        pl.semaphore_signal(barrier, inc=1, device_id={'cpo': peer // n_inner, 'cpi': lax.rem(peer, n_inner)}, device_id_type=MESH)
        return 0

    lax.fori_loop(1, n_dev, sig, 0)
    w_copies = [pltpu.make_async_copy(wout_hbm.at[:, pl.ds(n * wide, wide)], wbuf.at[n], w_sem) for n in range(n_w)]
    for cp in w_copies:
        cp.start()
    load.wait()
    pl.semaphore_wait(barrier, n_dev - 1)

    def k_tile(j):
        return qkv[pl.ds(j * kc, kc), 1].reshape(tk, head_dim)

    def vt_tile(j, rows):
        return jnp.concatenate([qkv[j * kc + u, 2] for u in range(rows // chunk)], axis=1)

    def q_strip(b, st):
        n = strip // chunk
        return qkv[pl.ds(b * qc + st * n, n), 0].reshape(strip, head_dim)

    def scores(dst, b, j, st):
        dst[:, st * strip:(st + 1) * strip] = lax.dot_general(k_tile(j), q_strip(b, st), (((1,), (1,)), ((), ())), preferred_element_type=F32)

    def update(src, j, st, rows, mask_off):
        sl = slice(st * strip, (st + 1) * strip)
        s = src[0:rows, sl]
        if mask_off is not None:
            r = lax.broadcasted_iota(jnp.int32, (rows, strip), 0)
            q = lax.broadcasted_iota(jnp.int32, (rows, strip), 1)
            s = jnp.where(r <= q + mask_off, s, NEG_BIG)
        m_old = m_ref[:, sl]
        m_new = jnp.maximum(m_old, jnp.max(s, axis=0, keepdims=True))
        alpha = jnp.exp2((m_old - m_new) * c_exp)
        p = jnp.exp2((s - m_new) * c_exp)
        l_ref[:, sl] = l_ref[:, sl] * alpha + jnp.sum(p, axis=0, keepdims=True)
        m_ref[:, sl] = m_new
        acc_ref[:, sl] = acc_ref[:, sl] * alpha + jnp.dot(vt_tile(j, rows), p.astype(BF16), preferred_element_type=F32)

    def q_block(n, _):
        row = lax.rem(y + 1 + n // 2, n_outer)
        b = jnp.where(lax.rem(n, 2) == 0, row, n_q - 1 - row)
        m_ref[...] = jnp.full(m_ref.shape, NEG_BIG, F32)
        l_ref[...] = jnp.zeros(l_ref.shape, F32)
        acc_ref[...] = jnp.zeros(acc_ref.shape, F32)
        for st in range(n_strips):
            scores(s0, b, 0, st)

        def pair(jj, _):
            for st in range(n_strips):
                scores(s1, b, 2 * jj + 1, st)
                update(s0, 2 * jj, st, tk, None)
            for st in range(n_strips):
                scores(s0, b, 2 * jj + 2, st)
                update(s1, 2 * jj + 1, st, tk, None)
            return 0

        lax.fori_loop(0, b, pair, 0)
        half = n_strips // 2
        for st in range(n_strips):
            if st >= half:
                scores(s1, b, 2 * b + 1, st)
                update(s0, 2 * b, st, tk, None)
            else:
                update(s0, 2 * b, st, (st + 1) * strip, st * strip)
        for st in range(half, n_strips):
            update(s1, 2 * b + 1, st, (st + 1 - half) * strip, (st - half) * strip)

        inv = 1.0 / l_ref[...]
        for u in range(qc):
            sl = slice(u * chunk, (u + 1) * chunk)
            o_stage[b * qc + u] = (acc_ref[:, sl] * inv[:, sl]).T.astype(BF16)
        cols = pl.ds(pl.multiple_of(me * head_dim, head_dim), head_dim)
        for u in range(qc):
            t = b * qc + u
            front = t < n_dev
            owner = jnp.where(front, t, 2 * n_dev - 1 - t)
            rows = pl.ds(pl.multiple_of(jnp.where(front, 0, chunk), chunk), chunk)

            @pl.when(owner == me)
            def _():
                o_recv[rows, cols] = o_stage[t]

            @pl.when(owner != me)
            def _():
                remote(o_stage.at[t], o_recv.at[rows, cols], o_send, o_sem, owner // n_inner, lax.rem(owner, n_inner)).start()
        return 0

    lax.fori_loop(0, n_q, q_block, 0)
    n_mine = 2 * (n_dev - 1)
    wait_bytes(o_stage.at[pl.ds(0, n_mine)], o_send)
    for cp in w_copies:
        pass
    wait_bytes(wbuf, w_sem)
    wait_bytes(o_stage.at[pl.ds(0, n_mine)], o_sem)

    def out_tile(n, _):
        out_ref[:, pl.ds(pl.multiple_of(n * wide, wide), wide)] = jnp.dot(o_recv[...], wbuf[n], preferred_element_type=F32).astype(BF16)
        return 0

    lax.fori_loop(0, n_w, out_tile, 0)


def solution(mesh):
    n_outer = mesh.shape['cpo']
    n_inner = mesh.shape['cpi']
    n_dev = n_outer * n_inner

    def device_step(hidden, w_query, w_key, w_value, w_out):
        rows, model_dim = hidden.shape
        chunk = rows // 2
        n_heads, head_dim = w_query.shape[1:]
        n_chunks = 2 * n_dev
        y = lax.axis_index('cpo')
        i = lax.axis_index('cpi')
        p = jnp.arange(PIECES, dtype=jnp.int32)
        rank = (y + piece_dy(p, n_outer)) % n_outer * n_inner + i
        t = jnp.where(piece_half(p) == 0, rank, n_chunks - 1 - rank)
        pos = t[:, None] * chunk + jnp.arange(chunk, dtype=jnp.int32)
        half_dim = head_dim // 2
        inv_freq = ROPE_BASE ** (-(2.0 / head_dim) * jnp.arange(half_dim, dtype=F32))
        angles = pos.astype(F32)[..., None] * inv_freq
        cos_t, sin_t = jnp.cos(angles), jnp.sin(angles)
        cos_t = jnp.concatenate([cos_t, cos_t], axis=-1)
        sin_t = jnp.concatenate([-sin_t, sin_t], axis=-1)

        any_spec = pl.BlockSpec(memory_space=pl.ANY)
        vmem_spec = pl.BlockSpec(memory_space=pltpu.VMEM)
        dma = pltpu.SemaphoreType.DMA
        qkv = pl.pallas_call(
            functools.partial(qkv_kernel, n_outer, n_inner),
            out_shape=jax.ShapeDtypeStruct((n_chunks, 3, chunk, head_dim), BF16),
            in_specs=[any_spec] * 4 + [vmem_spec] * 2,
            out_specs=any_spec,
            scratch_shapes=[
                pltpu.VMEM((PIECES, chunk, model_dim), BF16),
                pltpu.VMEM((4, 512, n_inner, head_dim), BF16),
                pltpu.VMEM((512, n_inner, head_dim), F32),
                pltpu.VMEM((n_inner // 2, model_dim, 6 * head_dim), BF16),
                pltpu.VMEM((PIECES, n_inner, 3, chunk, head_dim), BF16),
                pltpu.VMEM((PIECES, 2, 3, chunk, head_dim), BF16),
                dma((6,)), dma((PIECES,)), dma((2,)), dma((4,)), dma, dma, dma, dma((PIECES, 2)), dma,
            ],
            compiler_params=pltpu.CompilerParams(collective_id=0, has_side_effects=True, vmem_limit_bytes=60 * 2**20),
            name='qkv_exchange',
        )(hidden, w_query, w_key, w_value, cos_t, sin_t)

        tk, tq = 512, 1024
        n_w = 8
        return pl.pallas_call(
            functools.partial(attn_kernel, n_outer, n_inner, head_dim ** -0.5),
            out_shape=jax.ShapeDtypeStruct((rows, model_dim), BF16),
            in_specs=[any_spec] * 2,
            out_specs=vmem_spec,
            scratch_shapes=[
                pltpu.VMEM((n_chunks, 3, chunk, head_dim), BF16),
                pltpu.VMEM((n_w, n_heads * head_dim, model_dim // n_w), BF16),
                pltpu.VMEM((tk, tq), F32),
                pltpu.VMEM((tk, tq), F32),
                pltpu.VMEM((1, tq), F32),
                pltpu.VMEM((1, tq), F32),
                pltpu.VMEM((head_dim, tq), F32),
                pltpu.VMEM((n_chunks, chunk, head_dim), BF16),
                pltpu.VMEM((rows, n_heads * head_dim), BF16),
                dma, dma, dma, dma,
            ],
            compiler_params=pltpu.CompilerParams(collective_id=1, has_side_effects=True, vmem_limit_bytes=60 * 2**20),
            name='attn_out',
        )(qkv, w_out.reshape(n_heads * head_dim, model_dim))

    row_spec = P(('dp', 'cpo', 'cpi'), None)
    weight_spec = P(None, None, None)
    return jax.shard_map(device_step, mesh=mesh, in_specs=(row_spec, weight_spec, weight_spec, weight_spec, weight_spec), out_specs=row_spec, check_vma=False)
```

```python
import functools
import math

import jax
import jax.numpy as jnp
from jax import lax
from jax.experimental import pallas as pl
from jax.experimental.pallas import tpu as pltpu
from jax.sharding import PartitionSpec as P

ROPE_BASE = 500000.0
NEG_BIG = -1e30
MESH = pl.DeviceIdType.MESH
PIECES = 8
F32 = jnp.float32
BF16 = jnp.bfloat16


def remote(src, dst, send_sem, recv_sem, y, i):
    return pltpu.make_async_remote_copy(src_ref=src, dst_ref=dst, send_sem=send_sem, recv_sem=recv_sem, device_id={'cpo': y, 'cpi': i}, device_id_type=MESH)


def wait_bytes(ref, sem):
    pltpu.make_async_copy(ref, ref, sem).wait()


def piece_half(p):
    return jnp.where(p < 2, p, jnp.where(p < 4, 0, jnp.where(p < 6, 1, p - 6)))


def piece_dy(p, n_outer):
    return jnp.where(p < 2, 0, jnp.where(p < 6, jnp.where(lax.rem(p, 2) == 0, n_outer - 1, 1), 2))


def qkv_kernel(n_outer, n_inner, hid_in, wq, wk, wv, cos_ref, sin_ref, qkv_out,
               hid_buf, raw, wide, wbuf, stage, relay,
               h_send, h_recv, h_load, w_sem, s_send, l_sem, r_send, r_recv, q_recv):
    y = lax.axis_index('cpo')
    i = lax.axis_index('cpi')
    n_x = n_inner // 2
    x = i // 2
    c = lax.rem(i, 2)
    chunk = hid_buf.shape[1]
    n_chunks = qkv_out.shape[0]
    depth = raw.shape[1]
    n_k = wbuf.shape[1] // depth
    y_up = lax.rem(y + 1, n_outer)
    y_dn = lax.rem(y + n_outer - 1, n_outer)
    x_up = lax.rem(x + 1, n_x)
    x_dn = lax.rem(x + n_x - 1, n_x)
    weights = (wq, wk, wv)
    n_raw = raw.shape[0]

    def w_copy(t, kc, slot):
        src = weights[t].at[pl.ds(kc * depth, depth), pl.ds(pl.multiple_of(y * n_inner, n_inner), n_inner)]
        return pltpu.make_async_copy(src, raw.at[slot], w_sem.at[slot])

    for slot in range(n_raw):
        w_copy(0, slot, slot).start()
    own = [pltpu.make_async_copy(hid_in.at[pl.ds(f * chunk, chunk)], hid_buf.at[f], h_load.at[f]) for f in range(2)]
    for cp in own:
        cp.start()

    barrier = pltpu.get_barrier_semaphore()
    pl.semaphore_signal(barrier, inc=1, device_id={'cpo': y_up, 'cpi': i}, device_id_type=MESH)
    pl.semaphore_signal(barrier, inc=1, device_id={'cpo': y_dn, 'cpi': i}, device_id_type=MESH)
    for d in range(1, n_inner):
        pl.semaphore_signal(barrier, inc=1, device_id={'cpo': y, 'cpi': lax.rem(i + d, n_inner)}, device_id_type=MESH)
    pl.semaphore_wait(barrier, n_inner + 1)

    hid_sends = []
    for f in range(2):
        src = hid_in.at[pl.ds(f * chunk, chunk)]
        hid_sends.append(remote(src, hid_buf.at[2 + 2 * f], h_send.at[2 * f], h_recv.at[2 + 2 * f], y_up, i))
        hid_sends.append(remote(src, hid_buf.at[3 + 2 * f], h_send.at[2 * f + 1], h_recv.at[3 + 2 * f], y_dn, i))
    for cp in hid_sends:
        cp.start()
    fwd_up = remote(hid_buf.at[2], hid_buf.at[6], h_send.at[4], h_recv.at[6], y_up, i)
    fwd_dn = remote(hid_buf.at[5], hid_buf.at[7], h_send.at[5], h_recv.at[7], y_dn, i)

    for t in range(3):
        def relayout(kc, _, t=t):
            slot = lax.rem(t * n_k + kc, n_raw)
            w_copy(t, kc, slot).wait()
            wide[...] = raw[slot].astype(F32).reshape(wide.shape)
            for j in range(n_inner):
                col = (j % 2) * 384 + t * 128
                wbuf[j // 2, pl.ds(pl.multiple_of(kc * depth, depth), depth), col:col + 128] = wide[pl.ds(j, depth, n_inner), :].astype(BF16)
            nxt = kc + n_raw

            @pl.when(nxt < n_k)
            def _():
                w_copy(t, nxt, slot).start()

            if t < 2:
                @pl.when(nxt >= n_k)
                def _():
                    w_copy(t + 1, nxt - n_k, slot).start()
            return 0

        lax.fori_loop(0, n_k, relayout, 0)
    for cp in own:
        cp.wait()

    def chunk_index(p, src_i):
        rank = lax.rem(y + piece_dy(p, n_outer), n_outer) * n_inner + src_i
        return jnp.where(piece_half(p) == 0, rank, n_chunks - 1 - rank)

    def relay_copy(p, c2):
        front = piece_half(p) == 0
        src_x = jnp.where(front, x_dn, x_up)
        dst_x = jnp.where(front, x_up, x_dn)
        return remote(relay.at[p, c2], qkv_out.at[chunk_index(p, src_x * 2 + c)], r_send, q_recv, y, dst_x * 2 + c2)

    def forward_relay(p):
        for c2 in range(2):
            wait_bytes_remote = pltpu.make_async_copy(relay.at[p, c2], relay.at[p, c2], r_recv.at[p, c2])
            wait_bytes_remote.wait()
            relay_copy(p, c2).start()

    def piece(p, _):
        @pl.when(jnp.logical_and(p >= 2, p != 5))
        def _():
            wait_bytes(hid_buf.at[p], h_recv.at[p])

        @pl.when(p == 2)
        def _():
            fwd_up.start()

        @pl.when(p == 4)
        def _():
            wait_bytes(hid_buf.at[5], h_recv.at[5])
            fwd_dn.start()

        cos_p = cos_ref[p]
        sin_p = sin_ref[p]

        def rope(a):
            return a * cos_p + pltpu.roll(a, 64, 1) * sin_p

        out_t = chunk_index(p, i)

        def per_chip(kk, _):
            xc = lax.rem(x + jnp.where(kk == 0, 2, jnp.where(kk == 1, 1, jnp.where(kk == 2, n_x - 1, 0))), n_x)
            acc = jnp.dot(hid_buf[p], wbuf[xc], preferred_element_type=F32)
            for c2 in range(2):
                col = c2 * 384
                stage[p, xc * 2 + c2, 0] = rope(acc[:, col:col + 128]).astype(BF16)
                stage[p, xc * 2 + c2, 1] = rope(acc[:, col + 128:col + 256]).astype(BF16)
                stage[p, xc * 2 + c2, 2] = acc[:, col + 256:col + 384].T.astype(BF16)

            @pl.when(kk == 0)
            def _():
                via = jnp.where(piece_half(p) == 0, x_up, x_dn)
                for c2 in range(2):
                    remote(stage.at[p, xc * 2 + c2], relay.at[p, c2], s_send, r_recv.at[p, c2], y, via * 2 + c).start()

            @pl.when(jnp.logical_and(kk >= 1, kk <= 2))
            def _():
                for c2 in range(2):
                    remote(stage.at[p, xc * 2 + c2], qkv_out.at[out_t], s_send, q_recv, y, xc * 2 + c2).start()

            @pl.when(kk == 3)
            def _():
                remote(stage.at[p, xc * 2 + 1 - c], qkv_out.at[out_t], s_send, q_recv, y, xc * 2 + 1 - c).start()
                pltpu.make_async_copy(stage.at[p, i], qkv_out.at[out_t], l_sem).start()
            return 0

        lax.fori_loop(0, n_x, per_chip, 0)

        @pl.when(p >= 1)
        def _():
            forward_relay(p - 1)
        return 0

    lax.fori_loop(0, PIECES, piece, 0)
    forward_relay(PIECES - 1)

    for cp in hid_sends:
        cp.wait_send()
    fwd_up.wait_send()
    fwd_dn.wait_send()
    wait_bytes(stage.at[:, pl.ds(0, n_inner - 1)], s_send)
    wait_bytes(relay, r_send)
    wait_bytes(qkv_out.at[pl.ds(0, PIECES)], l_sem)
    wait_bytes(qkv_out.at[pl.ds(0, n_chunks - PIECES)], q_recv)


def attn_kernel(n_outer, n_inner, score_scale, qkv_hbm, wout_hbm, out_ref,
                qkv, wbuf, s0, s1, x0, x1, m_ref, l_ref, acc_ref, o_stage, o_recv, ld_sem, w_sem, o_send, o_sem):
    y = lax.axis_index('cpo')
    i = lax.axis_index('cpi')
    me = y * n_inner + i
    n_dev = n_outer * n_inner
    head_dim = qkv.shape[2]
    chunk = qkv.shape[3]
    tk, tq = s0.shape
    kc = tk // chunk
    qc = tq // chunk
    n_q = qkv.shape[0] // qc
    strip = 256
    n_strips = tq // strip
    n_w = wbuf.shape[0]
    wide = wbuf.shape[2]
    c_exp = score_scale * math.log2(math.e)

    load = pltpu.make_async_copy(qkv_hbm, qkv, ld_sem)
    load.start()

    barrier = pltpu.get_barrier_semaphore()

    def sig(d, _):
        peer = lax.rem(me + d, n_dev)
        pl.semaphore_signal(barrier, inc=1, device_id={'cpo': peer // n_inner, 'cpi': lax.rem(peer, n_inner)}, device_id_type=MESH)
        return 0

    lax.fori_loop(1, n_dev, sig, 0)
    w_copies = [pltpu.make_async_copy(wout_hbm.at[:, pl.ds(n * wide, wide)], wbuf.at[n], w_sem) for n in range(n_w)]
    for cp in w_copies:
        cp.start()
    load.wait()
    pl.semaphore_wait(barrier, n_dev - 1)

    def k_tile(j):
        return qkv[pl.ds(j * kc, kc), 1].reshape(tk, head_dim)

    def vt_tile(j, rows):
        return jnp.concatenate([qkv[j * kc + u, 2] for u in range(rows // chunk)], axis=1)

    def q_strip(b, st):
        n = strip // chunk
        return qkv[pl.ds(b * qc + st * n, n), 0].reshape(strip, head_dim)

    def scores(dst, mx, b, j, st, rows=tk, mask_off=None):
        sl = slice(st * strip, (st + 1) * strip)
        s = lax.dot_general(k_tile(j)[0:rows], q_strip(b, st), (((1,), (1,)), ((), ())), preferred_element_type=F32)
        if mask_off is not None:
            r = lax.broadcasted_iota(jnp.int32, (rows, strip), 0)
            q = lax.broadcasted_iota(jnp.int32, (rows, strip), 1)
            s = jnp.where(r <= q + mask_off, s, NEG_BIG)
        dst[0:rows, sl] = s
        mx[:, sl] = jnp.max(s, axis=0, keepdims=True)

    def update(src, mx, j, st, rows=tk):
        sl = slice(st * strip, (st + 1) * strip)
        m_old = m_ref[:, sl]
        m_new = jnp.maximum(m_old, mx[:, sl])
        alpha = jnp.exp2((m_old - m_new) * c_exp)
        p = jnp.exp2((src[0:rows, sl] - m_new) * c_exp)
        l_ref[:, sl] = l_ref[:, sl] * alpha + jnp.sum(p, axis=0, keepdims=True)
        m_ref[:, sl] = m_new
        acc_ref[:, sl] = acc_ref[:, sl] * alpha + jnp.dot(vt_tile(j, rows), p.astype(BF16), preferred_element_type=F32)

    def q_block(n, _):
        row = lax.rem(y + 1 + n // 2, n_outer)
        b = jnp.where(lax.rem(n, 2) == 0, row, n_q - 1 - row)
        m_ref[...] = jnp.full(m_ref.shape, NEG_BIG, F32)
        l_ref[...] = jnp.zeros(l_ref.shape, F32)
        acc_ref[...] = jnp.zeros(acc_ref.shape, F32)
        half = n_strips // 2

        def diag_scores(dst, mx, which, st):
            d = st - which * half
            if 0 <= d < half:
                scores(dst, mx, b, 2 * b + which, st, (d + 1) * strip, d * strip)
            elif d >= half:
                scores(dst, mx, b, 2 * b + which, st)

        def diag_update(src, mx, which, st):
            d = st - which * half
            if d >= 0:
                update(src, mx, 2 * b + which, st, min(d + 1, half) * strip)

        @pl.when(b > 0)
        def _():
            for st in range(n_strips):
                scores(s0, x0, b, 0, st)

        def pair(jj, _):
            for st in range(n_strips):
                scores(s1, x1, b, 2 * jj + 1, st)
                update(s0, x0, 2 * jj, st)
            for st in range(n_strips):
                scores(s0, x0, b, 2 * jj + 2, st)
                update(s1, x1, 2 * jj + 1, st)
            return 0

        lax.fori_loop(0, b - 1, pair, 0)

        @pl.when(b > 0)
        def _():
            for st in range(n_strips):
                scores(s1, x1, b, 2 * b - 1, st)
                update(s0, x0, 2 * b - 2, st)
            for st in range(n_strips):
                diag_scores(s0, x0, 0, st)
                update(s1, x1, 2 * b - 1, st)

        @pl.when(b == 0)
        def _():
            for st in range(n_strips):
                diag_scores(s0, x0, 0, st)

        for st in range(n_strips):
            diag_scores(s1, x1, 1, st)
            diag_update(s0, x0, 0, st)
        for st in range(n_strips):
            diag_update(s1, x1, 1, st)

        inv = 1.0 / l_ref[...]
        for u in range(qc):
            sl = slice(u * chunk, (u + 1) * chunk)
            o_stage[b * qc + u] = (acc_ref[:, sl] * inv[:, sl]).T.astype(BF16)
        cols = pl.ds(pl.multiple_of(me * head_dim, head_dim), head_dim)
        for u in range(qc):
            t = b * qc + u
            front = t < n_dev
            owner = jnp.where(front, t, 2 * n_dev - 1 - t)
            rows = pl.ds(pl.multiple_of(jnp.where(front, 0, chunk), chunk), chunk)

            @pl.when(owner == me)
            def _():
                o_recv[rows, cols] = o_stage[t]

            @pl.when(owner != me)
            def _():
                remote(o_stage.at[t], o_recv.at[rows, cols], o_send, o_sem, owner // n_inner, lax.rem(owner, n_inner)).start()
        return 0

    lax.fori_loop(0, n_q, q_block, 0)
    n_mine = 2 * (n_dev - 1)
    wait_bytes(o_stage.at[pl.ds(0, n_mine)], o_send)
    wait_bytes(wbuf, w_sem)
    wait_bytes(o_stage.at[pl.ds(0, n_mine)], o_sem)

    def out_tile(n, _):
        out_ref[:, pl.ds(pl.multiple_of(n * wide, wide), wide)] = jnp.dot(o_recv[...], wbuf[n], preferred_element_type=F32).astype(BF16)
        return 0

    lax.fori_loop(0, n_w, out_tile, 0)


def solution(mesh):
    n_outer = mesh.shape['cpo']
    n_inner = mesh.shape['cpi']
    n_dev = n_outer * n_inner

    def device_step(hidden, w_query, w_key, w_value, w_out):
        rows, model_dim = hidden.shape
        chunk = rows // 2
        n_heads, head_dim = w_query.shape[1:]
        n_chunks = 2 * n_dev
        y = lax.axis_index('cpo')
        i = lax.axis_index('cpi')
        p = jnp.arange(PIECES, dtype=jnp.int32)
        rank = (y + piece_dy(p, n_outer)) % n_outer * n_inner + i
        t = jnp.where(piece_half(p) == 0, rank, n_chunks - 1 - rank)
        pos = t[:, None] * chunk + jnp.arange(chunk, dtype=jnp.int32)
        half_dim = head_dim // 2
        inv_freq = ROPE_BASE ** (-(2.0 / head_dim) * jnp.arange(half_dim, dtype=F32))
        angles = pos.astype(F32)[..., None] * inv_freq
        cos_t, sin_t = jnp.cos(angles), jnp.sin(angles)
        cos_t = jnp.concatenate([cos_t, cos_t], axis=-1)
        sin_t = jnp.concatenate([-sin_t, sin_t], axis=-1)

        any_spec = pl.BlockSpec(memory_space=pl.ANY)
        vmem_spec = pl.BlockSpec(memory_space=pltpu.VMEM)
        dma = pltpu.SemaphoreType.DMA
        qkv = pl.pallas_call(
            functools.partial(qkv_kernel, n_outer, n_inner),
            out_shape=jax.ShapeDtypeStruct((n_chunks, 3, chunk, head_dim), BF16),
            in_specs=[any_spec] * 4 + [vmem_spec] * 2,
            out_specs=any_spec,
            scratch_shapes=[
                pltpu.VMEM((PIECES, chunk, model_dim), BF16),
                pltpu.VMEM((4, 512, n_inner, head_dim), BF16),
                pltpu.VMEM((512 * n_inner, head_dim), F32),
                pltpu.VMEM((n_inner // 2, model_dim, 6 * head_dim), BF16),
                pltpu.VMEM((PIECES, n_inner, 3, chunk, head_dim), BF16),
                pltpu.VMEM((PIECES, 2, 3, chunk, head_dim), BF16),
                dma((6,)), dma((PIECES,)), dma((2,)), dma((4,)), dma, dma, dma, dma((PIECES, 2)), dma,
            ],
            compiler_params=pltpu.CompilerParams(collective_id=0, has_side_effects=True, vmem_limit_bytes=60 * 2**20),
            name='qkv_exchange',
        )(hidden, w_query, w_key, w_value, cos_t, sin_t)

        tk, tq = 512, 1024
        n_w = 8
        return pl.pallas_call(
            functools.partial(attn_kernel, n_outer, n_inner, head_dim ** -0.5),
            out_shape=jax.ShapeDtypeStruct((rows, model_dim), BF16),
            in_specs=[any_spec] * 2,
            out_specs=vmem_spec,
            scratch_shapes=[
                pltpu.VMEM((n_chunks, 3, chunk, head_dim), BF16),
                pltpu.VMEM((n_w, n_heads * head_dim, model_dim // n_w), BF16),
                pltpu.VMEM((tk, tq), F32),
                pltpu.VMEM((tk, tq), F32),
                pltpu.VMEM((1, tq), F32),
                pltpu.VMEM((1, tq), F32),
                pltpu.VMEM((1, tq), F32),
                pltpu.VMEM((1, tq), F32),
                pltpu.VMEM((head_dim, tq), F32),
                pltpu.VMEM((n_chunks, chunk, head_dim), BF16),
                pltpu.VMEM((rows, n_heads * head_dim), BF16),
                dma, dma, dma, dma,
            ],
            compiler_params=pltpu.CompilerParams(collective_id=1, has_side_effects=True, vmem_limit_bytes=60 * 2**20),
            name='attn_out',
        )(qkv, w_out.reshape(n_heads * head_dim, model_dim))

    row_spec = P(('dp', 'cpo', 'cpi'), None)
    weight_spec = P(None, None, None)
    return jax.shard_map(device_step, mesh=mesh, in_specs=(row_spec, weight_spec, weight_spec, weight_spec, weight_spec), out_specs=row_spec, check_vma=False)
```

```python
import functools
import math

import jax
import jax.numpy as jnp
from jax import lax
from jax.experimental import pallas as pl
from jax.experimental.pallas import tpu as pltpu
from jax.sharding import PartitionSpec as P

ROPE_BASE = 500000.0
NEG_BIG = -1e30
MESH = pl.DeviceIdType.MESH
F32 = jnp.float32
BF16 = jnp.bfloat16

PIECES = 8
PIECE_HALF = (0, 1, 0, 0, 0, 1, 1, 1)
PIECE_DY = (0, 0, -1, 1, 2, -1, 1, 2)

PROJ, EARLY, FRONT, RECT, LAST = range(5)
STEPS = (
    (PROJ, 2), (PROJ, 3), (PROJ, 4), (EARLY, 0), (FRONT, 0), (FRONT, 1), (PROJ, 5), (PROJ, 6), (FRONT, 2), (PROJ, 7), (FRONT, 3),
    (RECT, -1), (RECT, 1), (RECT, 2), (LAST, 0), (LAST, 1), (LAST, 2), (LAST, 3),
)
STEP = {s: n for n, s in enumerate(STEPS)}
FORWARD = {STEP[PROJ, 3]: (2,), STEP[PROJ, 4]: (3,), STEP[EARLY, 0]: (4,), STEP[PROJ, 6]: (5,), STEP[FRONT, 2]: (6,), STEP[RECT, 1]: (7,)}
ARRIVE = {STEP[EARLY, 0]: (0, 1, 2, 3), STEP[FRONT, 0]: (4,), STEP[RECT, -1]: (5,), STEP[RECT, 1]: (6,), STEP[RECT, 2]: (7,)}


def lut(n, values):
    out = jnp.int32(values[-1])
    for k in range(len(values) - 2, -1, -1):
        if values[k] != values[k + 1] or k < len(values) - 2:
            out = jnp.where(n == k, jnp.int32(values[k]), out)
    return out


def remote(src, dst, send_sem, recv_sem, y, i):
    return pltpu.make_async_remote_copy(src_ref=src, dst_ref=dst, send_sem=send_sem, recv_sem=recv_sem, device_id={'cpo': y, 'cpi': i}, device_id_type=MESH)


def wait_bytes(ref, sem):
    pltpu.make_async_copy(ref, ref, sem).wait()


def layer_kernel(n_outer, n_inner, score_scale, hid_in, wq, wk, wv, wout, cos_ref, sin_ref, out_ref,
                 hid, raw, wide, big, stage, relay, qkv, s0, s1, x0, x1, m_ref, l_ref, acc_ref, o_recv,
                 h_send, h_recv, h_load, w_sem, s_send, r_send, r_recv, q_recv, wo_sem, o_send, o_sem):
    y = lax.axis_index('cpo')
    i = lax.axis_index('cpi')
    me = y * n_inner + i
    n_dev = n_outer * n_inner
    n_x = n_inner // 2
    x = i // 2
    c = lax.rem(i, 2)
    chunk, model_dim = hid.shape[1:]
    half_rows = chunk // 2
    head_dim = qkv.shape[2]
    n_chunks = qkv.shape[0]
    group = big.shape[2]
    depth = raw.shape[1]
    n_k = model_dim // depth
    n_raw = raw.shape[0]
    y_up = lax.rem(y + 1, n_outer)
    y_dn = lax.rem(y + n_outer - 1, n_outer)
    x_up = lax.rem(x + 1, n_x)
    x_dn = lax.rem(x + n_x - 1, n_x)
    x_far = lax.rem(x + 2, n_x)
    weights = (wq, wk, wv)
    tk, tq = s0.shape
    kc = tk // chunk
    qc = tq // chunk
    n_q = n_chunks // qc
    strip = 256
    n_strips = tq // strip
    half = n_strips // 2
    c_exp = score_scale * math.log2(math.e)

    def w_copy(t, k, slot):
        src = weights[t].at[pl.ds(k * depth, depth), pl.ds(pl.multiple_of(y * n_inner, n_inner), n_inner)]
        return pltpu.make_async_copy(src, raw.at[slot], w_sem.at[slot])

    for slot in range(n_raw):
        w_copy(0, slot, slot).start()
    own = [pltpu.make_async_copy(hid_in.at[pl.ds(f * chunk, chunk)], hid.at[f], h_load.at[f]) for f in range(2)]
    for cp in own:
        cp.start()

    barrier = pltpu.get_barrier_semaphore()

    def sig(d, _):
        peer = lax.rem(me + d, n_dev)
        pl.semaphore_signal(barrier, inc=1, device_id={'cpo': peer // n_inner, 'cpi': lax.rem(peer, n_inner)}, device_id_type=MESH)
        return 0

    lax.fori_loop(1, n_dev, sig, 0)
    pl.semaphore_wait(barrier, n_dev - 1)

    front = hid_in.at[pl.ds(0, chunk)]
    back = hid_in.at[pl.ds(chunk, chunk)]
    lo, hi = pl.ds(0, half_rows), pl.ds(half_rows, half_rows)
    send_front = [remote(front, hid.at[2], h_send.at[0], h_recv.at[2], y_up, i), remote(front, hid.at[3], h_send.at[1], h_recv.at[3], y_dn, i)]
    send_back = [remote(back, hid.at[5], h_send.at[2], h_recv.at[5], y_up, i), remote(back, hid.at[6], h_send.at[3], h_recv.at[6], y_dn, i)]
    fwd_front = [remote(hid.at[2, lo], hid.at[4, lo], h_send.at[4], h_recv.at[4], y_up, i), remote(hid.at[3, hi], hid.at[4, hi], h_send.at[5], h_recv.at[8], y_dn, i)]
    fwd_back = [remote(hid.at[5, lo], hid.at[7, lo], h_send.at[6], h_recv.at[7], y_up, i), remote(hid.at[6, hi], hid.at[7, hi], h_send.at[7], h_recv.at[9], y_dn, i)]
    for cp in send_front:
        cp.start()

    def chunk_index(p, src_i):
        rank = lax.rem(y + lut(p, PIECE_DY) + n_outer, n_outer) * n_inner + src_i
        return jnp.where(lut(p, PIECE_HALF) == 0, rank, n_chunks - 1 - rank)

    def forward_relay(p, t):
        for c2 in range(2):
            src_x, dst_x = (x_dn, x_up) if c2 == 0 else (x_up, x_dn)
            wait_bytes(relay.at[p, t, c2], r_recv.at[p, t, c2])
            remote(relay.at[p, t, c2], qkv.at[chunk_index(p, src_x * 2 + c), t], r_send, q_recv.at[p], y, dst_x * 2 + c2).start()

    def finish_heads(acc, p, t, j0):
        for u in range(acc.shape[1] // head_dim):
            a = acc[:, u * head_dim:(u + 1) * head_dim]
            if t < 2:
                stage[p, t, j0 + u] = (a * cos_ref[p] + pltpu.roll(a, head_dim // 2, 1) * sin_ref[p]).astype(BF16)
            else:
                stage[p, t, j0 + u] = a.T.astype(BF16)

    def send_piece(p, t):
        out_t = chunk_index(p, i)
        for c2 in range(2):
            via = x_up if c2 == 0 else x_dn
            remote(stage.at[p, t, x_far * 2 + c2], relay.at[p, t, c2], s_send, r_recv.at[p, t, c2], y, via * 2 + c).start()
        for xc in (x_up, x_dn):
            for c2 in range(2):
                remote(stage.at[p, t, xc * 2 + c2], qkv.at[out_t, t], s_send, q_recv.at[p], y, xc * 2 + c2).start()
        other = x * 2 + 1 - c
        remote(stage.at[p, t, other], qkv.at[out_t, t], s_send, q_recv.at[p], y, other).start()
        qkv[out_t, t] = stage[p, t, i]

    n_split = 2
    cols = group // n_split
    per_split = cols // head_dim

    for t in range(3):
        def relayout(k, _, t=t):
            slot = lax.rem(t * n_k + k, n_raw)
            w_copy(t, k, slot).wait()
            wide[...] = raw[slot].astype(F32).reshape(wide.shape)
            for j in range(n_inner):
                big[t, pl.ds(pl.multiple_of(k * depth, depth), depth), j * head_dim:(j + 1) * head_dim] = wide[pl.ds(j, depth, n_inner), :].astype(BF16)
            nxt = k + n_raw

            @pl.when(nxt < n_k)
            def _():
                w_copy(t, nxt, slot).start()

            if t < 2:
                @pl.when(nxt >= n_k)
                def _():
                    w_copy(t + 1, nxt - n_k, slot).start()
            return 0

        lax.fori_loop(0, n_k, relayout, 0)
        if t == 0:
            for cp in own:
                cp.wait()
        else:
            for p in range(2):
                forward_relay(p, t - 1)
        if t == 2:
            wait_bytes(hid.at[2], h_recv.at[2])
            wait_bytes(hid.at[3], h_recv.at[3])
            for cp in fwd_front + send_back:
                cp.start()

        def own_rows(n, _, t=t):
            w = big[t, :, pl.ds(pl.multiple_of(n * cols, cols), cols)]
            acc = jnp.dot(hid[0:2].reshape(2 * chunk, model_dim), w, preferred_element_type=F32)
            for p in range(2):
                finish_heads(acc[p * chunk:(p + 1) * chunk], p, t, n * per_split)
            return 0

        lax.fori_loop(0, n_split, own_rows, 0)
        for p in range(2):
            send_piece(p, t)

    def project(p):
        for t in range(3):
            for n in range(n_split):
                acc = jnp.dot(hid[p], big[t, :, n * cols:(n + 1) * cols], preferred_element_type=F32)
                finish_heads(acc, p, t, n * per_split)
            send_piece(p, t)

    def k_tile(j, rows):
        return qkv[pl.ds(j * kc, rows // chunk), 1].reshape(rows, head_dim)

    def vt_tile(j, rows):
        return jnp.concatenate([qkv[j * kc + u, 2] for u in range(rows // chunk)], axis=1)

    def q_strip(b, st):
        n = strip // chunk
        return qkv[pl.ds(b * qc + st * n, n), 0].reshape(strip, head_dim)

    def scores(dst, mx, b, j, st, rows=tk, mask_off=None):
        sl = slice(st * strip, (st + 1) * strip)
        s = lax.dot_general(k_tile(j, rows), q_strip(b, st), (((1,), (1,)), ((), ())), preferred_element_type=F32)
        if mask_off is not None:
            r = lax.broadcasted_iota(jnp.int32, (rows, strip), 0)
            q = lax.broadcasted_iota(jnp.int32, (rows, strip), 1)
            s = jnp.where(r <= q + mask_off, s, NEG_BIG)
        dst[0:rows, sl] = s
        mx[:, sl] = jnp.max(s, axis=0, keepdims=True)

    def update(src, mx, sidx, j, st, rows=tk):
        sl = slice(st * strip, (st + 1) * strip)
        m_old = m_ref[sidx, :, sl]
        m_new = jnp.maximum(m_old, mx[:, sl])
        alpha = jnp.exp2((m_old - m_new) * c_exp)
        p = jnp.exp2((src[0:rows, sl] - m_new) * c_exp)
        l_ref[sidx, :, sl] = l_ref[sidx, :, sl] * alpha + jnp.sum(p, axis=0, keepdims=True)
        m_ref[sidx, :, sl] = m_new
        acc_ref[sidx, :, sl] = acc_ref[sidx, :, sl] * alpha + jnp.dot(vt_tile(j, rows), p.astype(BF16), preferred_element_type=F32)

    def attend(b, sidx, n_kv, key_block, init, diag):
        @pl.when(init)
        def _():
            m_ref[sidx] = jnp.full(m_ref.shape[1:], NEG_BIG, F32)
            l_ref[sidx] = jnp.zeros(l_ref.shape[1:], F32)
            acc_ref[sidx] = jnp.zeros(acc_ref.shape[1:], F32)

        def diag_scores(dst, mx, which, st):
            d = st - which * half
            if 0 <= d < half:
                scores(dst, mx, b, 2 * b + which, st, (d + 1) * strip, d * strip)
            elif d >= half:
                scores(dst, mx, b, 2 * b + which, st)

        def diag_update(src, mx, which, st):
            d = st - which * half
            if d >= 0:
                update(src, mx, sidx, 2 * b + which, st, min(d + 1, half) * strip)

        @pl.when(n_kv > 0)
        def _():
            for st in range(n_strips):
                scores(s0, x0, b, 2 * key_block(0), st)

            def pair(jj, _):
                kb = key_block(jj)
                nxt = key_block(jj + 1)
                for st in range(n_strips):
                    scores(s1, x1, b, 2 * kb + 1, st)
                    update(s0, x0, sidx, 2 * kb, st)
                for st in range(n_strips):
                    scores(s0, x0, b, 2 * nxt, st)
                    update(s1, x1, sidx, 2 * kb + 1, st)
                return 0

            lax.fori_loop(0, n_kv - 1, pair, 0)
            kb = key_block(n_kv - 1)
            for st in range(n_strips):
                scores(s1, x1, b, 2 * kb + 1, st)
                update(s0, x0, sidx, 2 * kb, st)

            @pl.when(diag)
            def _():
                for st in range(n_strips):
                    diag_scores(s0, x0, 0, st)
                    update(s1, x1, sidx, 2 * kb + 1, st)

            @pl.when(jnp.logical_not(diag))
            def _():
                for st in range(n_strips):
                    update(s1, x1, sidx, 2 * kb + 1, st)

        @pl.when(n_kv == 0)
        def _():
            for st in range(n_strips):
                diag_scores(s0, x0, 0, st)

        @pl.when(diag)
        def _():
            for st in range(n_strips):
                diag_scores(s1, x1, 1, st)
                diag_update(s0, x0, 0, st)
            for st in range(n_strips):
                diag_update(s1, x1, 1, st)
            inv = 1.0 / l_ref[sidx]
            for u in range(qc):
                sl = slice(u * chunk, (u + 1) * chunk)
                qkv[b * qc + u, 0] = (acc_ref[sidx, :, sl] * inv[:, sl]).T.astype(BF16)

    o_cols = pl.ds(pl.multiple_of(me * head_dim, head_dim), head_dim)

    def send_out(b):
        def one(u, _):
            t = b * qc + u
            is_front = t < n_dev
            owner = jnp.where(is_front, t, 2 * n_dev - 1 - t)
            rows = pl.ds(pl.multiple_of(jnp.where(is_front, 0, chunk), chunk), chunk)

            @pl.when(owner == me)
            def _():
                o_recv[rows, o_cols] = qkv[t, 0]

            @pl.when(owner != me)
            def _():
                remote(qkv.at[t, 0], o_recv.at[rows, o_cols], o_send, o_sem.at[y], owner // n_inner, lax.rem(owner, n_inner)).start()
            return 0

        lax.fori_loop(0, qc, one, 0)

    def out_row(r):
        return lax.rem(y + 1 + r, n_outer)

    def wo_copies():
        res = []
        for r in range(n_outer - 1):
            for n in range(n_outer):
                src = wout.at[pl.ds(pl.multiple_of(out_row(r) * group, group), group), pl.ds(n * group, group)]
                res.append(pltpu.make_async_copy(src, big.at[r, pl.ds(n * group, group)], wo_sem.at[r]))
        for u in range(PIECES):
            src = wout.at[pl.ds(pl.multiple_of(y * group + u * chunk, chunk), chunk)]
            res.append(pltpu.make_async_copy(src, hid.at[u], wo_sem.at[n_outer - 1]))
        return res

    kinds = [k for k, _ in STEPS]
    args = [a for _, a in STEPS]

    def step(n, _):
        kind = lut(n, kinds)
        arg = lut(n, args)
        for m, ps in ARRIVE.items():
            @pl.when(n == m)
            def _(ps=ps):
                for p in ps:
                    wait_bytes(qkv.at[pl.ds(0, n_inner - 1)], q_recv.at[p])

        @pl.when(n == STEP[PROJ, 4])
        def _():
            wait_bytes(hid.at[4, lo], h_recv.at[4])
            wait_bytes(hid.at[4, hi], h_recv.at[8])

        @pl.when(n == STEP[PROJ, 5])
        def _():
            wait_bytes(hid.at[5], h_recv.at[5])
            wait_bytes(hid.at[6], h_recv.at[6])
            for cp in fwd_back:
                cp.start()

        @pl.when(n == STEP[PROJ, 7])
        def _():
            wait_bytes(hid.at[7, lo], h_recv.at[7])
            wait_bytes(hid.at[7, hi], h_recv.at[9])

        @pl.when(kind == PROJ)
        def _():
            project(arg)

        @pl.when(n == STEP[PROJ, 2])
        def _():
            for p in range(2):
                forward_relay(p, 2)

        @pl.when(n == STEP[PROJ, 7])
        def _():
            for cp in fwd_front + fwd_back:
                cp.wait_send()
            for cp in wo_copies():
                cp.start()

        @pl.when(kind != PROJ)
        def _():
            row = jnp.where(kind == EARLY, y, jnp.where(kind == RECT, lax.rem(y + arg + n_outer, n_outer), lax.rem(y + 1 + arg, n_outer)))
            b = jnp.where(kind == FRONT, row, n_q - 1 - row)
            own_last = jnp.logical_and(kind == LAST, row == y)
            n_kv = jnp.where(kind == EARLY, 3, jnp.where(kind == FRONT, row, jnp.where(kind == RECT, n_outer, n_outer - 1 - row + jnp.where(own_last, 1, 0))))

            def key_block(jj):
                early = lax.rem(y + jnp.where(jj == 0, 0, jnp.where(jj == 1, n_outer - 1, 1)), n_outer)
                last = jnp.where(own_last, jnp.where(jj == 0, lax.rem(y + 2, n_outer), n_outer - 1 + jj), n_outer + jj)
                return jnp.where(kind == EARLY, early, jnp.where(kind == LAST, last, jj))

            sidx = jnp.where(kind == FRONT, n_outer, row)
            attend(b, sidx, n_kv, key_block, kind != LAST, jnp.logical_or(kind == FRONT, kind == LAST))

            @pl.when(kind == LAST)
            def _():
                send_out(b)

        for m, ps in FORWARD.items():
            @pl.when(n == m)
            def _(ps=ps):
                for p in ps:
                    for t in range(3):
                        forward_relay(p, t)

        @pl.when(n == STEP[RECT, 1])
        def _():
            lax.fori_loop(0, n_outer, lambda k, _: (send_out(lax.rem(y + 1 + k, n_outer)), 0)[1], 0)
        return 0

    lax.fori_loop(0, len(STEPS), step, 0)

    def o_part(r):
        return o_recv[:, pl.ds(pl.multiple_of(out_row(r) * group, group), group)]

    rows = o_recv.shape[0]
    for r in range(n_outer - 1):
        wait_bytes(qkv.at[pl.ds(0, 2 * n_inner), 0], o_sem.at[out_row(r)])
        wait_bytes(big.at[r], wo_sem.at[r])
    per_buf = tk // rows

    def out_cols(n):
        return pl.ds(pl.multiple_of(n * group, group), group)

    for k, buf in enumerate((s0, s1)):
        def others(m, _, k=k, buf=buf):
            n = k * per_buf + m
            acc = None
            for r in range(n_outer - 1):
                d = jnp.dot(o_part(r), big[r, out_cols(n)], preferred_element_type=F32)
                acc = d if acc is None else acc + d
            buf[pl.ds(pl.multiple_of(m * rows, rows), rows)] = acc
            return 0

        lax.fori_loop(0, per_buf, others, 0)
    wait_bytes(qkv.at[pl.ds(0, 2 * (n_inner - 1)), 0], o_sem.at[y])
    wait_bytes(hid, wo_sem.at[n_outer - 1])
    for k, buf in enumerate((s0, s1)):
        def own_part(m, _, k=k, buf=buf):
            n = k * per_buf + m
            w = hid[:, :, out_cols(n)].reshape(group, group)
            acc = buf[pl.ds(pl.multiple_of(m * rows, rows), rows)] + jnp.dot(o_part(n_outer - 1), w, preferred_element_type=F32)
            out_ref[:, out_cols(n)] = acc.astype(BF16)
            return 0

        lax.fori_loop(0, per_buf, own_part, 0)

    for cp in send_front + send_back:
        cp.wait_send()
    wait_bytes(stage.at[:, :, pl.ds(0, n_inner - 1)], s_send)
    wait_bytes(relay, r_send)
    wait_bytes(qkv.at[pl.ds(0, 2 * (n_dev - 1)), 0], o_send)


def solution(mesh):
    n_outer = mesh.shape['cpo']
    n_inner = mesh.shape['cpi']
    n_dev = n_outer * n_inner

    def device_step(hidden, w_query, w_key, w_value, w_out):
        rows, model_dim = hidden.shape
        chunk = rows // 2
        n_heads, head_dim = w_query.shape[1:]
        n_chunks = 2 * n_dev
        y = lax.axis_index('cpo')
        i = lax.axis_index('cpi')
        rank = (y + jnp.array(PIECE_DY, jnp.int32)) % n_outer * n_inner + i
        t = jnp.where(jnp.array(PIECE_HALF, jnp.int32) == 0, rank, n_chunks - 1 - rank)
        pos = t[:, None] * chunk + jnp.arange(chunk, dtype=jnp.int32)
        half_dim = head_dim // 2
        inv_freq = ROPE_BASE ** (-(2.0 / head_dim) * jnp.arange(half_dim, dtype=F32))
        angles = pos.astype(F32)[..., None] * inv_freq
        cos_t, sin_t = jnp.cos(angles), jnp.sin(angles)
        cos_t = jnp.concatenate([cos_t, cos_t], axis=-1)
        sin_t = jnp.concatenate([-sin_t, sin_t], axis=-1)

        any_spec = pl.BlockSpec(memory_space=pl.ANY)
        vmem_spec = pl.BlockSpec(memory_space=pltpu.VMEM)
        dma = pltpu.SemaphoreType.DMA
        depth = 256
        tk, tq = 512, n_inner * chunk
        group = n_inner * head_dim
        return pl.pallas_call(
            functools.partial(layer_kernel, n_outer, n_inner, head_dim ** -0.5),
            out_shape=jax.ShapeDtypeStruct((rows, model_dim), BF16),
            in_specs=[any_spec] * 5 + [vmem_spec] * 2,
            out_specs=vmem_spec,
            scratch_shapes=[
                pltpu.VMEM((PIECES, chunk, model_dim), BF16),
                pltpu.VMEM((4, depth, n_inner, head_dim), BF16),
                pltpu.VMEM((depth * n_inner, head_dim), F32),
                pltpu.VMEM((3, model_dim, group), BF16),
                pltpu.VMEM((PIECES, 3, n_inner, chunk, head_dim), BF16),
                pltpu.VMEM((PIECES, 3, 2, chunk, head_dim), BF16),
                pltpu.VMEM((n_chunks, 3, chunk, head_dim), BF16),
                pltpu.VMEM((tk, tq), F32),
                pltpu.VMEM((tk, tq), F32),
                pltpu.VMEM((1, tq), F32),
                pltpu.VMEM((1, tq), F32),
                pltpu.VMEM((n_outer + 1, 1, tq), F32),
                pltpu.VMEM((n_outer + 1, 1, tq), F32),
                pltpu.VMEM((n_outer + 1, head_dim, tq), F32),
                pltpu.VMEM((rows, n_heads * head_dim), BF16),
                dma((8,)), dma((10,)), dma((2,)), dma((4,)), dma, dma, dma((PIECES, 3, 2)), dma((PIECES,)), dma((n_outer,)), dma, dma((n_outer,)),
            ],
            compiler_params=pltpu.CompilerParams(collective_id=0, has_side_effects=True, vmem_limit_bytes=63 * 2**20),
            name='layer',
        )(hidden, w_query, w_key, w_value, w_out.reshape(n_heads * head_dim, model_dim), cos_t, sin_t)

    row_spec = P(('dp', 'cpo', 'cpi'), None)
    weight_spec = P(None, None, None)
    return jax.shard_map(device_step, mesh=mesh, in_specs=(row_spec, weight_spec, weight_spec, weight_spec, weight_spec), out_specs=row_spec, check_vma=False)
```

```python
import functools
import math

import jax
import jax.numpy as jnp
from jax import lax
from jax.experimental import pallas as pl
from jax.experimental.pallas import tpu as pltpu
from jax.sharding import PartitionSpec as P

ROPE_BASE = 500000.0
NEG_BIG = -1e30
MESH = pl.DeviceIdType.MESH
F32 = jnp.float32
BF16 = jnp.bfloat16

PIECES = 8
PIECE_HALF = (0, 1, 0, 0, 0, 1, 1, 1)
PIECE_DY = (0, 0, -1, 1, 2, -1, 1, 2)

PROJ, EARLY, FRONT, RECT, LAST = range(5)
STEPS = (
    (PROJ, 2), (PROJ, 3), (EARLY, 0), (PROJ, 4), (EARLY, 1), (FRONT, 0), (FRONT, 1), (PROJ, 5), (PROJ, 6), (FRONT, 2), (PROJ, 7), (FRONT, 3),
    (RECT, -1), (RECT, 1), (RECT, 2), (LAST, 0), (LAST, 1), (LAST, 2), (LAST, 3),
)
STEP = {s: n for n, s in enumerate(STEPS)}
FORWARD = {STEP[PROJ, 3]: (2,), STEP[PROJ, 4]: (3,), STEP[EARLY, 1]: (4,), STEP[PROJ, 6]: (5,), STEP[FRONT, 2]: (6,), STEP[RECT, -1]: (7,)}
ARRIVE = {STEP[EARLY, 0]: (0, 1), STEP[EARLY, 1]: (2, 3), STEP[FRONT, 0]: (4,), STEP[RECT, -1]: (5,), STEP[RECT, 1]: (6,), STEP[RECT, 2]: (7,)}


def lut(n, values):
    out = jnp.int32(values[-1])
    for k in range(len(values) - 2, -1, -1):
        if values[k] != values[k + 1] or k < len(values) - 2:
            out = jnp.where(n == k, jnp.int32(values[k]), out)
    return out


def remote(src, dst, send_sem, recv_sem, y, i):
    return pltpu.make_async_remote_copy(src_ref=src, dst_ref=dst, send_sem=send_sem, recv_sem=recv_sem, device_id={'cpo': y, 'cpi': i}, device_id_type=MESH)


def wait_bytes(ref, sem):
    pltpu.make_async_copy(ref, ref, sem).wait()


def layer_kernel(n_outer, n_inner, score_scale, hid_in, wq, wk, wv, wout, cos_ref, sin_ref, out_ref,
                 hid, raw, wide, big, stage, relay, qkv, s0, s1, x0, x1, m_ref, l_ref, acc_ref, o_recv,
                 h_send, h_recv, h_load, w_sem, s_send, r_send, r_recv, q_recv, wo_sem, o_send, o_sem):
    y = lax.axis_index('cpo')
    i = lax.axis_index('cpi')
    me = y * n_inner + i
    n_dev = n_outer * n_inner
    n_x = n_inner // 2
    x = i // 2
    c = lax.rem(i, 2)
    chunk, model_dim = hid.shape[1:]
    half_rows = chunk // 2
    head_dim = qkv.shape[2]
    n_chunks = qkv.shape[0]
    group = big.shape[2]
    depth = raw.shape[1]
    n_k = model_dim // depth
    n_raw = raw.shape[0]
    y_up = lax.rem(y + 1, n_outer)
    y_dn = lax.rem(y + n_outer - 1, n_outer)
    x_up = lax.rem(x + 1, n_x)
    x_dn = lax.rem(x + n_x - 1, n_x)
    x_far = lax.rem(x + 2, n_x)
    weights = (wq, wk, wv)
    tk, tq = s0.shape
    kc = tk // chunk
    qc = tq // chunk
    n_q = n_chunks // qc
    strip = 256
    n_strips = tq // strip
    half = n_strips // 2
    c_exp = score_scale * math.log2(math.e)

    def w_copy(t, k, slot):
        src = weights[t].at[pl.ds(k * depth, depth), pl.ds(pl.multiple_of(y * n_inner, n_inner), n_inner)]
        return pltpu.make_async_copy(src, raw.at[slot], w_sem.at[slot])

    for slot in range(n_raw):
        w_copy(0, slot, slot).start()
    own = [pltpu.make_async_copy(hid_in.at[pl.ds(f * chunk, chunk)], hid.at[f], h_load.at[f]) for f in range(2)]
    for cp in own:
        cp.start()

    barrier = pltpu.get_barrier_semaphore()

    def sig(d, _):
        peer = lax.rem(me + d, n_dev)
        pl.semaphore_signal(barrier, inc=1, device_id={'cpo': peer // n_inner, 'cpi': lax.rem(peer, n_inner)}, device_id_type=MESH)
        return 0

    lax.fori_loop(1, n_dev, sig, 0)

    front = hid_in.at[pl.ds(0, chunk)]
    back = hid_in.at[pl.ds(chunk, chunk)]
    lo, hi = pl.ds(0, half_rows), pl.ds(half_rows, half_rows)
    send_front = [remote(front, hid.at[2], h_send.at[0], h_recv.at[2], y_up, i), remote(front, hid.at[3], h_send.at[1], h_recv.at[3], y_dn, i)]
    send_back = [remote(back, hid.at[5], h_send.at[2], h_recv.at[5], y_up, i), remote(back, hid.at[6], h_send.at[3], h_recv.at[6], y_dn, i)]
    fwd_front = [remote(hid.at[2, lo], hid.at[4, lo], h_send.at[4], h_recv.at[4], y_up, i), remote(hid.at[3, hi], hid.at[4, hi], h_send.at[5], h_recv.at[8], y_dn, i)]
    fwd_back = [remote(hid.at[5, lo], hid.at[7, lo], h_send.at[6], h_recv.at[7], y_up, i), remote(hid.at[6, hi], hid.at[7, hi], h_send.at[7], h_recv.at[9], y_dn, i)]

    def chunk_index(p, src_i):
        rank = lax.rem(y + lut(p, PIECE_DY) + n_outer, n_outer) * n_inner + src_i
        return jnp.where(lut(p, PIECE_HALF) == 0, rank, n_chunks - 1 - rank)

    def forward_relay(p, t):
        for c2 in range(2):
            src_x, dst_x = (x_dn, x_up) if c2 == 0 else (x_up, x_dn)
            wait_bytes(relay.at[p, t, c2], r_recv.at[p, t, c2])
            remote(relay.at[p, t, c2], qkv.at[chunk_index(p, src_x * 2 + c), t], r_send, q_recv.at[p], y, dst_x * 2 + c2).start()

    def finish_heads(acc, p, t, j0):
        for u in range(acc.shape[1] // head_dim):
            a = acc[:, u * head_dim:(u + 1) * head_dim]
            if t < 2:
                stage[p, t, j0 + u] = (a * cos_ref[p] + pltpu.roll(a, head_dim // 2, 1) * sin_ref[p]).astype(BF16)
            else:
                stage[p, t, j0 + u] = a.T.astype(BF16)

    def send_piece(p, t):
        out_t = chunk_index(p, i)
        for c2 in range(2):
            via = x_up if c2 == 0 else x_dn
            remote(stage.at[p, t, x_far * 2 + c2], relay.at[p, t, c2], s_send, r_recv.at[p, t, c2], y, via * 2 + c).start()
        for xc in (x_up, x_dn):
            for c2 in range(2):
                remote(stage.at[p, t, xc * 2 + c2], qkv.at[out_t, t], s_send, q_recv.at[p], y, xc * 2 + c2).start()
        other = x * 2 + 1 - c
        remote(stage.at[p, t, other], qkv.at[out_t, t], s_send, q_recv.at[p], y, other).start()
        qkv[out_t, t] = stage[p, t, i]

    n_split = 2
    cols = group // n_split
    per_split = cols // head_dim

    for t in range(3):
        def relayout(k, _, t=t):
            slot = lax.rem(t * n_k + k, n_raw)
            w_copy(t, k, slot).wait()
            wide[...] = raw[slot].astype(F32).reshape(wide.shape)
            for j in range(n_inner):
                big[t, pl.ds(pl.multiple_of(k * depth, depth), depth), j * head_dim:(j + 1) * head_dim] = wide[pl.ds(j, depth, n_inner), :].astype(BF16)
            nxt = k + n_raw

            @pl.when(nxt < n_k)
            def _():
                w_copy(t, nxt, slot).start()

            if t < 2:
                @pl.when(nxt >= n_k)
                def _():
                    w_copy(t + 1, nxt - n_k, slot).start()
            return 0

        lax.fori_loop(0, n_k, relayout, 0)
        if t == 0:
            pl.semaphore_wait(barrier, n_dev - 1)
            for cp in send_front:
                cp.start()
            for cp in own:
                cp.wait()
        else:
            for p in range(2):
                forward_relay(p, t - 1)
        def own_rows(n, _, t=t):
            w = big[t, :, pl.ds(pl.multiple_of(n * cols, cols), cols)]
            acc = jnp.dot(hid[0:2].reshape(2 * chunk, model_dim), w, preferred_element_type=F32)
            for p in range(2):
                finish_heads(acc[p * chunk:(p + 1) * chunk], p, t, n * per_split)
            return 0

        lax.fori_loop(0, n_split, own_rows, 0)
        for p in range(2):
            send_piece(p, t)

    wait_bytes(hid.at[2], h_recv.at[2])
    wait_bytes(hid.at[3], h_recv.at[3])
    for cp in fwd_front + send_back:
        cp.start()

    def project(p):
        for t in range(3):
            for n in range(n_split):
                acc = jnp.dot(hid[p], big[t, :, n * cols:(n + 1) * cols], preferred_element_type=F32)
                finish_heads(acc, p, t, n * per_split)
            send_piece(p, t)

    def k_tile(j, rows):
        return qkv[pl.ds(j * kc, rows // chunk), 1].reshape(rows, head_dim)

    def vt_tile(j, rows):
        return jnp.concatenate([qkv[j * kc + u, 2] for u in range(rows // chunk)], axis=1)

    def q_strip(b, st):
        n = strip // chunk
        return qkv[pl.ds(b * qc + st * n, n), 0].reshape(strip, head_dim)

    def scores(dst, mx, b, j, st, rows=tk, mask_off=None):
        sl = slice(st * strip, (st + 1) * strip)
        s = lax.dot_general(k_tile(j, rows), q_strip(b, st), (((1,), (1,)), ((), ())), preferred_element_type=F32)
        if mask_off is not None:
            r = lax.broadcasted_iota(jnp.int32, (rows, strip), 0)
            q = lax.broadcasted_iota(jnp.int32, (rows, strip), 1)
            s = jnp.where(r <= q + mask_off, s, NEG_BIG)
        dst[0:rows, sl] = s
        mx[:, sl] = jnp.max(s, axis=0, keepdims=True)

    def update(src, mx, sidx, j, st, rows=tk):
        sl = slice(st * strip, (st + 1) * strip)
        m_old = m_ref[sidx, :, sl]
        m_new = jnp.maximum(m_old, mx[:, sl])
        alpha = jnp.exp2((m_old - m_new) * c_exp)
        p = jnp.exp2((src[0:rows, sl] - m_new) * c_exp)
        l_ref[sidx, :, sl] = l_ref[sidx, :, sl] * alpha + jnp.sum(p, axis=0, keepdims=True)
        m_ref[sidx, :, sl] = m_new
        acc_ref[sidx, :, sl] = acc_ref[sidx, :, sl] * alpha + jnp.dot(vt_tile(j, rows), p.astype(BF16), preferred_element_type=F32)

    def attend(b, sidx, n_kv, key_block, init, diag, finish):
        @pl.when(init)
        def _():
            m_ref[sidx] = jnp.full(m_ref.shape[1:], NEG_BIG, F32)
            l_ref[sidx] = jnp.zeros(l_ref.shape[1:], F32)
            acc_ref[sidx] = jnp.zeros(acc_ref.shape[1:], F32)

        def diag_scores(dst, mx, which, st):
            d = st - which * half
            if 0 <= d < half:
                scores(dst, mx, b, 2 * b + which, st, (d + 1) * strip, d * strip)
            elif d >= half:
                scores(dst, mx, b, 2 * b + which, st)

        def diag_update(src, mx, which, st):
            d = st - which * half
            if d >= 0:
                update(src, mx, sidx, 2 * b + which, st, min(d + 1, half) * strip)

        @pl.when(n_kv > 0)
        def _():
            for st in range(n_strips):
                scores(s0, x0, b, 2 * key_block(0), st)

            def pair(jj, _):
                kb = key_block(jj)
                nxt = key_block(jj + 1)
                for st in range(n_strips):
                    scores(s1, x1, b, 2 * kb + 1, st)
                    update(s0, x0, sidx, 2 * kb, st)
                for st in range(n_strips):
                    scores(s0, x0, b, 2 * nxt, st)
                    update(s1, x1, sidx, 2 * kb + 1, st)
                return 0

            lax.fori_loop(0, n_kv - 1, pair, 0)
            kb = key_block(n_kv - 1)
            for st in range(n_strips):
                scores(s1, x1, b, 2 * kb + 1, st)
                update(s0, x0, sidx, 2 * kb, st)

            @pl.when(diag)
            def _():
                for st in range(n_strips):
                    diag_scores(s0, x0, 0, st)
                    update(s1, x1, sidx, 2 * kb + 1, st)

            @pl.when(jnp.logical_not(diag))
            def _():
                for st in range(n_strips):
                    update(s1, x1, sidx, 2 * kb + 1, st)

        @pl.when(n_kv == 0)
        def _():
            for st in range(n_strips):
                diag_scores(s0, x0, 0, st)

        @pl.when(diag)
        def _():
            for st in range(n_strips):
                diag_scores(s1, x1, 1, st)
                diag_update(s0, x0, 0, st)
            for st in range(n_strips):
                diag_update(s1, x1, 1, st)

        @pl.when(finish)
        def _():
            inv = 1.0 / l_ref[sidx]
            for u in range(qc):
                sl = slice(u * chunk, (u + 1) * chunk)
                qkv[b * qc + u, 0] = (acc_ref[sidx, :, sl] * inv[:, sl]).T.astype(BF16)

    o_cols = pl.ds(pl.multiple_of(me * head_dim, head_dim), head_dim)

    def send_out(b):
        def one(u, _):
            t = b * qc + u
            is_front = t < n_dev
            owner = jnp.where(is_front, t, 2 * n_dev - 1 - t)
            rows = pl.ds(pl.multiple_of(jnp.where(is_front, 0, chunk), chunk), chunk)

            @pl.when(owner == me)
            def _():
                o_recv[rows, o_cols] = qkv[t, 0]

            @pl.when(owner != me)
            def _():
                remote(qkv.at[t, 0], o_recv.at[rows, o_cols], o_send, o_sem.at[y], owner // n_inner, lax.rem(owner, n_inner)).start()
            return 0

        lax.fori_loop(0, qc, one, 0)

    def out_row(r):
        return lax.rem(y + 1 + r, n_outer)

    def wo_copies():
        res = []
        for r in range(n_outer - 1):
            for n in range(n_outer):
                src = wout.at[pl.ds(pl.multiple_of(out_row(r) * group, group), group), pl.ds(n * group, group)]
                res.append(pltpu.make_async_copy(src, big.at[r, pl.ds(n * group, group)], wo_sem.at[r]))
        for u in range(PIECES):
            src = wout.at[pl.ds(pl.multiple_of(y * group + u * chunk, chunk), chunk)]
            res.append(pltpu.make_async_copy(src, hid.at[u], wo_sem.at[n_outer - 1]))
        return res

    kinds = [k for k, _ in STEPS]
    args = [a for _, a in STEPS]

    def step(n, _):
        kind = lut(n, kinds)
        arg = lut(n, args)
        for m, ps in ARRIVE.items():
            @pl.when(n == m)
            def _(ps=ps):
                for p in ps:
                    wait_bytes(qkv.at[pl.ds(0, n_inner - 1)], q_recv.at[p])

        @pl.when(n == STEP[PROJ, 4])
        def _():
            wait_bytes(hid.at[4, lo], h_recv.at[4])
            wait_bytes(hid.at[4, hi], h_recv.at[8])

        @pl.when(n == STEP[PROJ, 5])
        def _():
            wait_bytes(hid.at[5], h_recv.at[5])
            wait_bytes(hid.at[6], h_recv.at[6])
            for cp in fwd_back:
                cp.start()

        @pl.when(n == STEP[PROJ, 7])
        def _():
            wait_bytes(hid.at[7, lo], h_recv.at[7])
            wait_bytes(hid.at[7, hi], h_recv.at[9])

        @pl.when(kind == PROJ)
        def _():
            project(arg)

        @pl.when(n == STEP[PROJ, 2])
        def _():
            for p in range(2):
                forward_relay(p, 2)

        @pl.when(n == STEP[PROJ, 7])
        def _():
            for cp in fwd_front + fwd_back:
                cp.wait_send()
            for cp in wo_copies():
                cp.start()

        @pl.when(kind != PROJ)
        def _():
            row = jnp.where(kind == EARLY, y, jnp.where(kind == RECT, lax.rem(y + arg + n_outer, n_outer), lax.rem(y + 1 + arg, n_outer)))
            b = jnp.where(kind == FRONT, row, n_q - 1 - row)
            own_last = jnp.logical_and(kind == LAST, row == y)
            n_early = jnp.where(arg == 0, 1, 2)
            n_last = n_outer - 1 - row + jnp.where(own_last, 1, 0)
            n_kv = jnp.where(kind == EARLY, n_early, jnp.where(kind == FRONT, row, jnp.where(kind == RECT, n_outer, n_last)))

            def key_block(jj):
                early = jnp.where(arg == 0, y, jnp.where(jj == 0, y_dn, y_up))
                last = jnp.where(own_last, jnp.where(jj == 0, lax.rem(y + 2, n_outer), n_outer - 1 + jj), n_outer + jj)
                return jnp.where(kind == EARLY, early, jnp.where(kind == LAST, last, jj))

            sidx = jnp.where(kind == FRONT, n_outer, row)
            finish = jnp.logical_or(kind == FRONT, kind == LAST)
            init = jnp.logical_and(kind != LAST, jnp.logical_not(jnp.logical_and(kind == EARLY, arg == 1)))
            diag = jnp.logical_or(jnp.logical_and(finish, jnp.logical_not(own_last)), jnp.logical_and(kind == EARLY, arg == 0))
            attend(b, sidx, n_kv, key_block, init, diag, finish)

            @pl.when(finish)
            def _():
                send_out(b)

        for m, ps in FORWARD.items():
            @pl.when(n == m)
            def _(ps=ps):
                for p in ps:
                    for t in range(3):
                        forward_relay(p, t)

        return 0

    lax.fori_loop(0, len(STEPS), step, 0)

    def o_part(r):
        return o_recv[:, pl.ds(pl.multiple_of(out_row(r) * group, group), group)]

    rows = o_recv.shape[0]
    for r in range(n_outer - 1):
        wait_bytes(qkv.at[pl.ds(0, 2 * n_inner), 0], o_sem.at[out_row(r)])
        wait_bytes(big.at[r], wo_sem.at[r])
    per_buf = tk // rows

    def out_cols(n):
        return pl.ds(pl.multiple_of(n * group, group), group)

    for k, buf in enumerate((s0, s1)):
        def others(m, _, k=k, buf=buf):
            n = k * per_buf + m
            acc = None
            for r in range(n_outer - 1):
                d = jnp.dot(o_part(r), big[r, out_cols(n)], preferred_element_type=F32)
                acc = d if acc is None else acc + d
            buf[pl.ds(pl.multiple_of(m * rows, rows), rows)] = acc
            return 0

        lax.fori_loop(0, per_buf, others, 0)
    wait_bytes(qkv.at[pl.ds(0, 2 * (n_inner - 1)), 0], o_sem.at[y])
    wait_bytes(hid, wo_sem.at[n_outer - 1])
    for k, buf in enumerate((s0, s1)):
        def own_part(m, _, k=k, buf=buf):
            n = k * per_buf + m
            w = hid[:, :, out_cols(n)].reshape(group, group)
            acc = buf[pl.ds(pl.multiple_of(m * rows, rows), rows)] + jnp.dot(o_part(n_outer - 1), w, preferred_element_type=F32)
            out_ref[:, out_cols(n)] = acc.astype(BF16)
            return 0

        lax.fori_loop(0, per_buf, own_part, 0)

    for cp in send_front + send_back:
        cp.wait_send()
    wait_bytes(stage.at[:, :, pl.ds(0, n_inner - 1)], s_send)
    wait_bytes(relay, r_send)
    wait_bytes(qkv.at[pl.ds(0, 2 * (n_dev - 1)), 0], o_send)


def solution(mesh):
    n_outer = mesh.shape['cpo']
    n_inner = mesh.shape['cpi']
    n_dev = n_outer * n_inner

    def device_step(hidden, w_query, w_key, w_value, w_out):
        rows, model_dim = hidden.shape
        chunk = rows // 2
        n_heads, head_dim = w_query.shape[1:]
        n_chunks = 2 * n_dev
        y = lax.axis_index('cpo')
        i = lax.axis_index('cpi')
        rank = (y + jnp.array(PIECE_DY, jnp.int32)) % n_outer * n_inner + i
        t = jnp.where(jnp.array(PIECE_HALF, jnp.int32) == 0, rank, n_chunks - 1 - rank)
        pos = t[:, None] * chunk + jnp.arange(chunk, dtype=jnp.int32)
        half_dim = head_dim // 2
        lane = jnp.arange(head_dim, dtype=jnp.int32)
        inv_freq = ROPE_BASE ** (-(2.0 / head_dim) * (lane % half_dim).astype(F32))
        angles = pos.astype(F32)[..., None] * inv_freq
        cos_t = jnp.cos(angles)
        sin_t = jnp.sin(angles) * jnp.where(lane < half_dim, -1.0, 1.0)

        any_spec = pl.BlockSpec(memory_space=pl.ANY)
        vmem_spec = pl.BlockSpec(memory_space=pltpu.VMEM)
        dma = pltpu.SemaphoreType.DMA
        depth = 256
        tk, tq = 512, n_inner * chunk
        group = n_inner * head_dim
        return pl.pallas_call(
            functools.partial(layer_kernel, n_outer, n_inner, head_dim ** -0.5),
            out_shape=jax.ShapeDtypeStruct((rows, model_dim), BF16),
            in_specs=[any_spec] * 5 + [vmem_spec] * 2,
            out_specs=vmem_spec,
            scratch_shapes=[
                pltpu.VMEM((PIECES, chunk, model_dim), BF16),
                pltpu.VMEM((4, depth, n_inner, head_dim), BF16),
                pltpu.VMEM((depth * n_inner, head_dim), F32),
                pltpu.VMEM((3, model_dim, group), BF16),
                pltpu.VMEM((PIECES, 3, n_inner, chunk, head_dim), BF16),
                pltpu.VMEM((PIECES, 3, 2, chunk, head_dim), BF16),
                pltpu.VMEM((n_chunks, 3, chunk, head_dim), BF16),
                pltpu.VMEM((tk, tq), F32),
                pltpu.VMEM((tk, tq), F32),
                pltpu.VMEM((1, tq), F32),
                pltpu.VMEM((1, tq), F32),
                pltpu.VMEM((n_outer + 1, 1, tq), F32),
                pltpu.VMEM((n_outer + 1, 1, tq), F32),
                pltpu.VMEM((n_outer + 1, head_dim, tq), F32),
                pltpu.VMEM((rows, n_heads * head_dim), BF16),
                dma((8,)), dma((10,)), dma((2,)), dma((4,)), dma, dma, dma((PIECES, 3, 2)), dma((PIECES,)), dma((n_outer,)), dma, dma((n_outer,)),
            ],
            compiler_params=pltpu.CompilerParams(collective_id=0, has_side_effects=True, vmem_limit_bytes=63 * 2**20),
            name='layer',
        )(hidden, w_query, w_key, w_value, w_out.reshape(n_heads * head_dim, model_dim), cos_t, sin_t)

    row_spec = P(('dp', 'cpo', 'cpi'), None)
    weight_spec = P(None, None, None)
    return jax.shard_map(device_step, mesh=mesh, in_specs=(row_spec, weight_spec, weight_spec, weight_spec, weight_spec), out_specs=row_spec, check_vma=False)
```

```python
import functools
import math

import jax
import jax.numpy as jnp
from jax import lax
from jax.experimental import pallas as pl
from jax.experimental.pallas import tpu as pltpu
from jax.sharding import PartitionSpec as P

ROPE_BASE = 500000.0
NEG_BIG = -1e30
MESH = pl.DeviceIdType.MESH
F32 = jnp.float32
BF16 = jnp.bfloat16

PIECES = 8
PIECE_HALF = (0, 1, 0, 0, 0, 1, 1, 1)
PIECE_DY = (0, 0, -1, 1, 2, -1, 1, 2)

PROJ, EARLY, FRONT, RECT, LAST = range(5)
STEPS = (
    (PROJ, 2), (PROJ, 3), (EARLY, 0), (PROJ, 4), (EARLY, 1), (FRONT, 0), (FRONT, 1), (PROJ, 5), (PROJ, 6), (FRONT, 2), (PROJ, 7), (FRONT, 3),
    (RECT, -1), (RECT, 1), (RECT, 2), (LAST, 0), (LAST, 1), (LAST, 2), (LAST, 3),
)
STEP = {s: n for n, s in enumerate(STEPS)}
ROW_SHIFT = (2, 1, -1, 0)
FORWARD = {STEP[PROJ, 3]: (2,), STEP[PROJ, 4]: (3,), STEP[PROJ, 6]: (5,), STEP[FRONT, 2]: (6,), STEP[RECT, -1]: (7,)}
ARRIVE = {STEP[EARLY, 0]: (0, 1), STEP[EARLY, 1]: (2, 3), STEP[FRONT, 0]: (4,), STEP[RECT, -1]: (5,), STEP[RECT, 1]: (6,), STEP[RECT, 2]: (7,)}


def lut(n, values):
    out = jnp.int32(values[-1])
    for k in range(len(values) - 2, -1, -1):
        if values[k] != values[k + 1] or k < len(values) - 2:
            out = jnp.where(n == k, jnp.int32(values[k]), out)
    return out


def remote(src, dst, send_sem, recv_sem, y, i):
    return pltpu.make_async_remote_copy(src_ref=src, dst_ref=dst, send_sem=send_sem, recv_sem=recv_sem, device_id={'cpo': y, 'cpi': i}, device_id_type=MESH)


def wait_bytes(ref, sem):
    pltpu.make_async_copy(ref, ref, sem).wait()


def layer_kernel(n_outer, n_inner, score_scale, hid_in, wq, wk, wv, wout, cos_ref, sin_ref, out_ref,
                 hid, raw, wide, big, stage, relay, qkv, s0, s1, x0, x1, m_ref, l_ref, acc_ref, o_recv,
                 h_send, h_recv, h_load, w_sem, s_send, r_send, r_recv, q_recv, wo_sem, o_send, o_sem):
    y = lax.axis_index('cpo')
    i = lax.axis_index('cpi')
    me = y * n_inner + i
    n_dev = n_outer * n_inner
    n_x = n_inner // 2
    x = i // 2
    c = lax.rem(i, 2)
    chunk, model_dim = hid.shape[1:]
    half_rows = chunk // 2
    head_dim = qkv.shape[2]
    n_chunks = qkv.shape[0]
    group = big.shape[2]
    depth = raw.shape[1]
    n_k = model_dim // depth
    n_raw = raw.shape[0]
    y_up = lax.rem(y + 1, n_outer)
    y_dn = lax.rem(y + n_outer - 1, n_outer)
    x_up = lax.rem(x + 1, n_x)
    x_dn = lax.rem(x + n_x - 1, n_x)
    x_far = lax.rem(x + 2, n_x)
    weights = (wq, wk, wv)
    tk, tq = s0.shape
    kc = tk // chunk
    qc = tq // chunk
    n_q = n_chunks // qc
    strip = 256
    n_strips = tq // strip
    half = n_strips // 2
    c_exp = score_scale * math.log2(math.e)

    def w_copy(t, k, slot):
        src = weights[t].at[pl.ds(k * depth, depth), pl.ds(pl.multiple_of(y * n_inner, n_inner), n_inner)]
        return pltpu.make_async_copy(src, raw.at[slot], w_sem.at[slot])

    for slot in range(n_raw):
        w_copy(0, slot, slot).start()
    own = [pltpu.make_async_copy(hid_in.at[pl.ds(f * chunk, chunk)], hid.at[f], h_load.at[f]) for f in range(2)]
    for cp in own:
        cp.start()

    barrier = pltpu.get_barrier_semaphore()

    def sig(d, _):
        peer = lax.rem(me + d, n_dev)
        pl.semaphore_signal(barrier, inc=1, device_id={'cpo': peer // n_inner, 'cpi': lax.rem(peer, n_inner)}, device_id_type=MESH)
        return 0

    lax.fori_loop(1, n_dev, sig, 0)

    front = hid_in.at[pl.ds(0, chunk)]
    back = hid_in.at[pl.ds(chunk, chunk)]
    lo, hi = pl.ds(0, half_rows), pl.ds(half_rows, half_rows)
    send_front = [remote(front, hid.at[2], h_send.at[0], h_recv.at[2], y_up, i), remote(front, hid.at[3], h_send.at[1], h_recv.at[3], y_dn, i)]
    send_back = [remote(back, hid.at[5], h_send.at[2], h_recv.at[5], y_up, i), remote(back, hid.at[6], h_send.at[3], h_recv.at[6], y_dn, i)]
    fwd_front = [remote(hid.at[2, lo], hid.at[4, lo], h_send.at[4], h_recv.at[4], y_up, i), remote(hid.at[3, hi], hid.at[4, hi], h_send.at[5], h_recv.at[8], y_dn, i)]
    fwd_back = [remote(hid.at[5, lo], hid.at[7, lo], h_send.at[6], h_recv.at[7], y_up, i), remote(hid.at[6, hi], hid.at[7, hi], h_send.at[7], h_recv.at[9], y_dn, i)]

    def chunk_index(p, src_i):
        rank = lax.rem(y + lut(p, PIECE_DY) + n_outer, n_outer) * n_inner + src_i
        return jnp.where(lut(p, PIECE_HALF) == 0, rank, n_chunks - 1 - rank)

    def forward_relay(p, t):
        for c2 in range(2):
            src_x, dst_x = (x_dn, x_up) if c2 == 0 else (x_up, x_dn)
            wait_bytes(relay.at[p, t, c2], r_recv.at[p, t, c2])
            remote(relay.at[p, t, c2], qkv.at[chunk_index(p, src_x * 2 + c), t], r_send, q_recv.at[p], y, dst_x * 2 + c2).start()

    def finish_heads(acc, p, t, j0):
        for u in range(acc.shape[1] // head_dim):
            a = acc[:, u * head_dim:(u + 1) * head_dim]
            if t < 2:
                stage[p, t, j0 + u] = (a * cos_ref[p] + pltpu.roll(a, head_dim // 2, 1) * sin_ref[p]).astype(BF16)
            else:
                stage[p, t, j0 + u] = a.T.astype(BF16)

    def send_piece(p, t):
        out_t = chunk_index(p, i)
        for c2 in range(2):
            via = x_up if c2 == 0 else x_dn
            remote(stage.at[p, t, x_far * 2 + c2], relay.at[p, t, c2], s_send, r_recv.at[p, t, c2], y, via * 2 + c).start()
        for xc in (x_up, x_dn):
            for c2 in range(2):
                remote(stage.at[p, t, xc * 2 + c2], qkv.at[out_t, t], s_send, q_recv.at[p], y, xc * 2 + c2).start()
        other = x * 2 + 1 - c
        remote(stage.at[p, t, other], qkv.at[out_t, t], s_send, q_recv.at[p], y, other).start()
        qkv[out_t, t] = stage[p, t, i]

    n_split = 2
    cols = group // n_split
    per_split = cols // head_dim

    for t in range(3):
        def relayout(k, _, t=t):
            slot = lax.rem(t * n_k + k, n_raw)
            w_copy(t, k, slot).wait()
            wide[...] = raw[slot].astype(F32).reshape(wide.shape)
            for j in range(n_inner):
                big[t, pl.ds(pl.multiple_of(k * depth, depth), depth), j * head_dim:(j + 1) * head_dim] = wide[pl.ds(j, depth, n_inner), :].astype(BF16)
            nxt = k + n_raw

            @pl.when(nxt < n_k)
            def _():
                w_copy(t, nxt, slot).start()

            if t < 2:
                @pl.when(nxt >= n_k)
                def _():
                    w_copy(t + 1, nxt - n_k, slot).start()
            return 0

        with jax.named_scope(f'relayout{t}'):
            lax.fori_loop(0, n_k, relayout, 0)
        if t == 0:
            with jax.named_scope('barrier'):
                pl.semaphore_wait(barrier, n_dev - 1)
            for cp in send_front:
                cp.start()
            for cp in own:
                cp.wait()
        else:
            for p in range(2):
                with jax.named_scope(f'ownrelay{t}'):
                    forward_relay(p, t - 1)
        def own_rows(n, _, t=t):
            w = big[t, :, pl.ds(pl.multiple_of(n * cols, cols), cols)]
            acc = jnp.dot(hid[0:2].reshape(2 * chunk, model_dim), w, preferred_element_type=F32)
            for p in range(2):
                finish_heads(acc[p * chunk:(p + 1) * chunk], p, t, n * per_split)
            return 0

        with jax.named_scope(f'own{t}'):
            lax.fori_loop(0, n_split, own_rows, 0)
        for p in range(2):
            send_piece(p, t)

    with jax.named_scope('hid23'):
        wait_bytes(hid.at[2], h_recv.at[2])
        wait_bytes(hid.at[3], h_recv.at[3])
    for cp in fwd_front + send_back:
        cp.start()

    def project(p):
        for t in range(3):
            for n in range(n_split):
                acc = jnp.dot(hid[p], big[t, :, n * cols:(n + 1) * cols], preferred_element_type=F32)
                finish_heads(acc, p, t, n * per_split)
            send_piece(p, t)

    def k_tile(j, rows):
        return qkv[pl.ds(j * kc, rows // chunk), 1].reshape(rows, head_dim)

    def vt_tile(j, rows):
        return jnp.concatenate([qkv[j * kc + u, 2] for u in range(rows // chunk)], axis=1)

    def q_strip(b, st):
        n = strip // chunk
        return qkv[pl.ds(b * qc + st * n, n), 0].reshape(strip, head_dim)

    def scores(dst, mx, b, j, st, rows=tk, mask_off=None):
        sl = slice(st * strip, (st + 1) * strip)
        s = lax.dot_general(k_tile(j, rows), q_strip(b, st), (((1,), (1,)), ((), ())), preferred_element_type=F32)
        if mask_off is not None:
            r = lax.broadcasted_iota(jnp.int32, (rows, strip), 0)
            q = lax.broadcasted_iota(jnp.int32, (rows, strip), 1)
            s = jnp.where(r <= q + mask_off, s, NEG_BIG)
        dst[0:rows, sl] = s
        mx[:, sl] = jnp.max(s, axis=0, keepdims=True)

    def update(src, mx, sidx, j, st, rows=tk):
        sl = slice(st * strip, (st + 1) * strip)
        m_old = m_ref[sidx, :, sl]
        m_new = jnp.maximum(m_old, mx[:, sl])
        alpha = jnp.exp2((m_old - m_new) * c_exp)
        p = jnp.exp2((src[0:rows, sl] - m_new) * c_exp)
        l_ref[sidx, :, sl] = l_ref[sidx, :, sl] * alpha + jnp.sum(p, axis=0, keepdims=True)
        m_ref[sidx, :, sl] = m_new
        acc_ref[sidx, :, sl] = acc_ref[sidx, :, sl] * alpha + jnp.dot(vt_tile(j, rows), p.astype(BF16), preferred_element_type=F32)

    def attend(b, sidx, n_kv, key_block, init, diag, finish):
        @pl.when(init)
        def _():
            m_ref[sidx] = jnp.full(m_ref.shape[1:], NEG_BIG, F32)
            l_ref[sidx] = jnp.zeros(l_ref.shape[1:], F32)
            acc_ref[sidx] = jnp.zeros(acc_ref.shape[1:], F32)

        def diag_scores(dst, mx, which, st):
            d = st - which * half
            if 0 <= d < half:
                scores(dst, mx, b, 2 * b + which, st, (d + 1) * strip, d * strip)
            elif d >= half:
                scores(dst, mx, b, 2 * b + which, st)

        def diag_update(src, mx, which, st):
            d = st - which * half
            if d >= 0:
                update(src, mx, sidx, 2 * b + which, st, min(d + 1, half) * strip)

        @pl.when(n_kv > 0)
        def _():
            for st in range(n_strips):
                scores(s0, x0, b, 2 * key_block(0), st)

            def pair(jj, _):
                kb = key_block(jj)
                nxt = key_block(jj + 1)
                for st in range(n_strips):
                    scores(s1, x1, b, 2 * kb + 1, st)
                    update(s0, x0, sidx, 2 * kb, st)
                for st in range(n_strips):
                    scores(s0, x0, b, 2 * nxt, st)
                    update(s1, x1, sidx, 2 * kb + 1, st)
                return 0

            lax.fori_loop(0, n_kv - 1, pair, 0)
            kb = key_block(n_kv - 1)
            for st in range(n_strips):
                scores(s1, x1, b, 2 * kb + 1, st)
                update(s0, x0, sidx, 2 * kb, st)

            @pl.when(diag)
            def _():
                for st in range(n_strips):
                    diag_scores(s0, x0, 0, st)
                    update(s1, x1, sidx, 2 * kb + 1, st)

            @pl.when(jnp.logical_not(diag))
            def _():
                for st in range(n_strips):
                    update(s1, x1, sidx, 2 * kb + 1, st)

        @pl.when(n_kv == 0)
        def _():
            for st in range(n_strips):
                diag_scores(s0, x0, 0, st)

        @pl.when(diag)
        def _():
            for st in range(n_strips):
                diag_scores(s1, x1, 1, st)
                diag_update(s0, x0, 0, st)
            for st in range(n_strips):
                diag_update(s1, x1, 1, st)

        @pl.when(finish)
        def _():
            inv = 1.0 / l_ref[sidx]
            for u in range(qc):
                sl = slice(u * chunk, (u + 1) * chunk)
                qkv[b * qc + u, 0] = (acc_ref[sidx, :, sl] * inv[:, sl]).T.astype(BF16)

    o_cols = pl.ds(pl.multiple_of(me * head_dim, head_dim), head_dim)

    def send_out(b):
        def one(u, _):
            t = b * qc + u
            is_front = t < n_dev
            owner = jnp.where(is_front, t, 2 * n_dev - 1 - t)
            rows = pl.ds(pl.multiple_of(jnp.where(is_front, 0, chunk), chunk), chunk)

            @pl.when(owner == me)
            def _():
                o_recv[rows, o_cols] = qkv[t, 0]

            @pl.when(owner != me)
            def _():
                remote(qkv.at[t, 0], o_recv.at[rows, o_cols], o_send, o_sem.at[y], owner // n_inner, lax.rem(owner, n_inner)).start()
            return 0

        lax.fori_loop(0, qc, one, 0)

    def out_row(r):
        return lax.rem(y + 1 + r, n_outer)

    def wo_copies():
        res = []
        for r in range(n_outer - 1):
            for n in range(n_outer):
                src = wout.at[pl.ds(pl.multiple_of(out_row(r) * group, group), group), pl.ds(n * group, group)]
                res.append(pltpu.make_async_copy(src, big.at[r, pl.ds(n * group, group)], wo_sem.at[r]))
        for u in range(PIECES):
            src = wout.at[pl.ds(pl.multiple_of(y * group + u * chunk, chunk), chunk)]
            res.append(pltpu.make_async_copy(src, hid.at[u], wo_sem.at[n_outer - 1]))
        return res

    kinds = [k for k, _ in STEPS]
    args = [a for _, a in STEPS]

    def step(n, _):
        kind = lut(n, kinds)
        arg = lut(n, args)
        for m, ps in ARRIVE.items():
            @pl.when(n == m)
            def _(ps=ps):
                with jax.named_scope(f'arrive{ps[0]}'):
                    for p in ps:
                        wait_bytes(qkv.at[pl.ds(0, n_inner - 1)], q_recv.at[p])

        @pl.when(n == STEP[PROJ, 4])
        def _():
            with jax.named_scope('hid4'):
                wait_bytes(hid.at[4, lo], h_recv.at[4])
                wait_bytes(hid.at[4, hi], h_recv.at[8])

        @pl.when(n == STEP[EARLY, 1])
        def _():
            with jax.named_scope('forward4'):
                for t in range(3):
                    forward_relay(4, t)

        @pl.when(n == STEP[PROJ, 5])
        def _():
            with jax.named_scope('hid56'):
                wait_bytes(hid.at[5], h_recv.at[5])
                wait_bytes(hid.at[6], h_recv.at[6])
            for cp in fwd_back:
                cp.start()

        @pl.when(n == STEP[PROJ, 7])
        def _():
            with jax.named_scope('hid7'):
                wait_bytes(hid.at[7, lo], h_recv.at[7])
                wait_bytes(hid.at[7, hi], h_recv.at[9])

        @pl.when(kind == PROJ)
        def _():
            with jax.named_scope('project'):
                project(arg)

        @pl.when(n == STEP[PROJ, 2])
        def _():
            with jax.named_scope('ownrelay3'):
                for p in range(2):
                    forward_relay(p, 2)

        @pl.when(n == STEP[PROJ, 7])
        def _():
            for cp in fwd_front + fwd_back:
                cp.wait_send()
            for cp in wo_copies():
                cp.start()
            for k in range(3):
                send_out(lax.rem(y + ROW_SHIFT[k] + n_outer, n_outer))

        @pl.when(kind != PROJ)
        def _():
            shift = jnp.where(kind == EARLY, 0, jnp.where(kind == RECT, arg, lut(arg, ROW_SHIFT)))
            row = lax.rem(y + shift + n_outer, n_outer)
            b = jnp.where(kind == FRONT, row, n_q - 1 - row)
            own_last = jnp.logical_and(kind == LAST, row == y)
            n_early = jnp.where(arg == 0, 1, 2)
            n_last = n_outer - 1 - row + jnp.where(own_last, 1, 0)
            n_kv = jnp.where(kind == EARLY, n_early, jnp.where(kind == FRONT, row, jnp.where(kind == RECT, n_outer, n_last)))

            def key_block(jj):
                early = jnp.where(arg == 0, y, jnp.where(jj == 0, y_dn, y_up))
                last = jnp.where(own_last, jnp.where(jj == 0, lax.rem(y + 2, n_outer), n_outer - 1 + jj), n_outer + jj)
                return jnp.where(kind == EARLY, early, jnp.where(kind == LAST, last, jj))

            sidx = jnp.where(kind == FRONT, n_outer, row)
            finish = jnp.logical_or(kind == FRONT, kind == LAST)
            init = jnp.logical_and(kind != LAST, jnp.logical_not(jnp.logical_and(kind == EARLY, arg == 1)))
            diag = jnp.logical_or(jnp.logical_and(finish, jnp.logical_not(own_last)), jnp.logical_and(kind == EARLY, arg == 0))
            with jax.named_scope('attend'):
                attend(b, sidx, n_kv, key_block, init, diag, finish)

            @pl.when(jnp.logical_and(finish, n > STEP[PROJ, 7]))
            def _():
                send_out(b)

        for m, ps in FORWARD.items():
            @pl.when(n == m)
            def _(ps=ps):
                with jax.named_scope(f'forward{ps[0]}'):
                    for p in ps:
                        for t in range(3):
                            forward_relay(p, t)

        return 0

    lax.fori_loop(0, len(STEPS), step, 0)

    def o_part(r):
        return o_recv[:, pl.ds(pl.multiple_of(out_row(r) * group, group), group)]

    rows = o_recv.shape[0]
    for r in range(n_outer - 1):
        with jax.named_scope(f'owait{r}'):
            wait_bytes(qkv.at[pl.ds(0, 2 * n_inner), 0], o_sem.at[out_row(r)])
            wait_bytes(big.at[r], wo_sem.at[r])
    per_buf = tk // rows

    def out_cols(n):
        return pl.ds(pl.multiple_of(n * group, group), group)

    for k, buf in enumerate((s0, s1)):
        def others(m, _, k=k, buf=buf):
            n = k * per_buf + m
            acc = None
            for r in range(n_outer - 1):
                d = jnp.dot(o_part(r), big[r, out_cols(n)], preferred_element_type=F32)
                acc = d if acc is None else acc + d
            buf[pl.ds(pl.multiple_of(m * rows, rows), rows)] = acc
            return 0

        with jax.named_scope(f'oproj{k}'):
            lax.fori_loop(0, per_buf, others, 0)
    with jax.named_scope('owaitown'):
        wait_bytes(qkv.at[pl.ds(0, 2 * (n_inner - 1)), 0], o_sem.at[y])
    wait_bytes(hid, wo_sem.at[n_outer - 1])
    for k, buf in enumerate((s0, s1)):
        def own_part(m, _, k=k, buf=buf):
            n = k * per_buf + m
            w = hid[:, :, out_cols(n)].reshape(group, group)
            acc = buf[pl.ds(pl.multiple_of(m * rows, rows), rows)] + jnp.dot(o_part(n_outer - 1), w, preferred_element_type=F32)
            out_ref[:, out_cols(n)] = acc.astype(BF16)
            return 0

        with jax.named_scope(f'oprojown{k}'):
            lax.fori_loop(0, per_buf, own_part, 0)

    for cp in send_front + send_back:
        cp.wait_send()
    wait_bytes(stage.at[:, :, pl.ds(0, n_inner - 1)], s_send)
    wait_bytes(relay, r_send)
    wait_bytes(qkv.at[pl.ds(0, 2 * (n_dev - 1)), 0], o_send)


def solution(mesh):
    n_outer = mesh.shape['cpo']
    n_inner = mesh.shape['cpi']
    n_dev = n_outer * n_inner

    def device_step(hidden, w_query, w_key, w_value, w_out):
        rows, model_dim = hidden.shape
        chunk = rows // 2
        n_heads, head_dim = w_query.shape[1:]
        n_chunks = 2 * n_dev
        y = lax.axis_index('cpo')
        i = lax.axis_index('cpi')
        rank = (y + jnp.array(PIECE_DY, jnp.int32)) % n_outer * n_inner + i
        t = jnp.where(jnp.array(PIECE_HALF, jnp.int32) == 0, rank, n_chunks - 1 - rank)
        pos = t[:, None] * chunk + jnp.arange(chunk, dtype=jnp.int32)
        half_dim = head_dim // 2
        lane = jnp.arange(head_dim, dtype=jnp.int32)
        inv_freq = ROPE_BASE ** (-(2.0 / head_dim) * (lane % half_dim).astype(F32))
        angles = pos.astype(F32)[..., None] * inv_freq
        cos_t = jnp.cos(angles)
        sin_t = jnp.sin(angles) * jnp.where(lane < half_dim, -1.0, 1.0)

        any_spec = pl.BlockSpec(memory_space=pl.ANY)
        vmem_spec = pl.BlockSpec(memory_space=pltpu.VMEM)
        dma = pltpu.SemaphoreType.DMA
        depth = 256
        tk, tq = 512, n_inner * chunk
        group = n_inner * head_dim
        return pl.pallas_call(
            functools.partial(layer_kernel, n_outer, n_inner, head_dim ** -0.5),
            out_shape=pltpu.VMEM((rows, model_dim), BF16),
            in_specs=[any_spec] * 5 + [vmem_spec] * 2,
            out_specs=vmem_spec,
            scratch_shapes=[
                pltpu.VMEM((PIECES, chunk, model_dim), BF16),
                pltpu.VMEM((4, depth, n_inner, head_dim), BF16),
                pltpu.VMEM((depth * n_inner, head_dim), F32),
                pltpu.VMEM((3, model_dim, group), BF16),
                pltpu.VMEM((PIECES, 3, n_inner, chunk, head_dim), BF16),
                pltpu.VMEM((PIECES, 3, 2, chunk, head_dim), BF16),
                pltpu.VMEM((n_chunks, 3, chunk, head_dim), BF16),
                pltpu.VMEM((tk, tq), F32),
                pltpu.VMEM((tk, tq), F32),
                pltpu.VMEM((1, tq), F32),
                pltpu.VMEM((1, tq), F32),
                pltpu.VMEM((n_outer + 1, 1, tq), F32),
                pltpu.VMEM((n_outer + 1, 1, tq), F32),
                pltpu.VMEM((n_outer + 1, head_dim, tq), F32),
                pltpu.VMEM((rows, n_heads * head_dim), BF16),
                dma((8,)), dma((10,)), dma((2,)), dma((4,)), dma, dma, dma((PIECES, 3, 2)), dma((PIECES,)), dma((n_outer,)), dma, dma((n_outer,)),
            ],
            compiler_params=pltpu.CompilerParams(collective_id=0, has_side_effects=True, vmem_limit_bytes=60 * 2**20),
            name='layer',
        )(hidden, w_query, w_key, w_value, w_out.reshape(n_heads * head_dim, model_dim), cos_t, sin_t)

    row_spec = P(('dp', 'cpo', 'cpi'), None)
    weight_spec = P(None, None, None)
    return jax.shard_map(device_step, mesh=mesh, in_specs=(row_spec, weight_spec, weight_spec, weight_spec, weight_spec), out_specs=row_spec, check_vma=False)
```

```python
import functools
import math

import jax
import jax.numpy as jnp
from jax import lax
from jax.experimental import pallas as pl
from jax.experimental.pallas import tpu as pltpu
from jax.sharding import PartitionSpec as P

ROPE_BASE = 500000.0
NEG_BIG = -1e30
MESH = pl.DeviceIdType.MESH
F32 = jnp.float32
BF16 = jnp.bfloat16

PIECES = 8
PIECE_HALF = (0, 1, 0, 0, 0, 1, 1, 1)
PIECE_DY = (0, 0, -1, 1, 2, -1, 1, 2)

PROJ, EARLY, FRONT, RECT, LAST = range(5)
STEPS = (
    (PROJ, 2), (PROJ, 3), (EARLY, 0), (PROJ, 4), (EARLY, 1), (FRONT, 0), (FRONT, 1), (PROJ, 5), (PROJ, 6), (FRONT, 2), (PROJ, 7), (FRONT, 3),
    (RECT, -1), (RECT, 1), (RECT, 2), (LAST, 0), (LAST, 1), (LAST, 2), (LAST, 3),
)
STEP = {s: n for n, s in enumerate(STEPS)}
ROW_SHIFT = (2, 1, -1, 0)
FORWARD = {STEP[EARLY, 1]: (4,), STEP[FRONT, 3]: (7,)}
ARRIVE = {STEP[EARLY, 0]: (0, 1), STEP[EARLY, 1]: (2, 3), STEP[FRONT, 0]: (4,), STEP[RECT, -1]: (5,), STEP[RECT, 1]: (6,), STEP[RECT, 2]: (7,)}


def lut(n, values):
    out = jnp.int32(values[-1])
    for k in range(len(values) - 2, -1, -1):
        if values[k] != values[k + 1] or k < len(values) - 2:
            out = jnp.where(n == k, jnp.int32(values[k]), out)
    return out


def remote(src, dst, send_sem, recv_sem, y, i):
    return pltpu.make_async_remote_copy(src_ref=src, dst_ref=dst, send_sem=send_sem, recv_sem=recv_sem, device_id={'cpo': y, 'cpi': i}, device_id_type=MESH)


def wait_bytes(ref, sem):
    pltpu.make_async_copy(ref, ref, sem).wait()


def layer_kernel(n_outer, n_inner, score_scale, hid_in, wq, wk, wv, wout, cos_ref, sin_ref, out_ref,
                 hid, raw, wide, big, stage, relay, qkv, s0, s1, x0, x1, m_ref, l_ref, acc_ref, o_recv,
                 h_send, h_recv, h_load, w_sem, s_send, r_send, r_recv, q_recv, wo_sem, o_send, o_sem):
    y = lax.axis_index('cpo')
    i = lax.axis_index('cpi')
    me = y * n_inner + i
    n_dev = n_outer * n_inner
    n_x = n_inner // 2
    x = i // 2
    c = lax.rem(i, 2)
    chunk, model_dim = hid.shape[1:]
    half_rows = chunk // 2
    head_dim = qkv.shape[2]
    n_chunks = qkv.shape[0]
    group = big.shape[2]
    depth = raw.shape[1]
    n_k = model_dim // depth
    n_raw = raw.shape[0]
    y_up = lax.rem(y + 1, n_outer)
    y_dn = lax.rem(y + n_outer - 1, n_outer)
    x_up = lax.rem(x + 1, n_x)
    x_dn = lax.rem(x + n_x - 1, n_x)
    x_far = lax.rem(x + 2, n_x)
    weights = (wq, wk, wv)
    tk, tq = s0.shape
    kc = tk // chunk
    qc = tq // chunk
    n_q = n_chunks // qc
    strip = 256
    n_strips = tq // strip
    half = n_strips // 2
    c_exp = score_scale * math.log2(math.e)

    def w_copy(t, k, slot):
        src = weights[t].at[pl.ds(k * depth, depth), pl.ds(pl.multiple_of(y * n_inner, n_inner), n_inner)]
        return pltpu.make_async_copy(src, raw.at[slot], w_sem.at[slot])

    for slot in range(n_raw):
        w_copy(0, slot, slot).start()
    own = [pltpu.make_async_copy(hid_in.at[pl.ds(f * chunk, chunk)], hid.at[f], h_load.at[f]) for f in range(2)]
    for cp in own:
        cp.start()

    barrier = pltpu.get_barrier_semaphore()

    def sig(d, _):
        peer = lax.rem(me + d, n_dev)
        pl.semaphore_signal(barrier, inc=1, device_id={'cpo': peer // n_inner, 'cpi': lax.rem(peer, n_inner)}, device_id_type=MESH)
        return 0

    lax.fori_loop(1, n_dev, sig, 0)

    front = hid_in.at[pl.ds(0, chunk)]
    back = hid_in.at[pl.ds(chunk, chunk)]
    lo, hi = pl.ds(0, half_rows), pl.ds(half_rows, half_rows)
    send_front = [remote(front, hid.at[2], h_send.at[0], h_recv.at[2], y_up, i), remote(front, hid.at[3], h_send.at[1], h_recv.at[3], y_dn, i)]
    send_back = [remote(back, hid.at[5], h_send.at[2], h_recv.at[5], y_up, i), remote(back, hid.at[6], h_send.at[3], h_recv.at[6], y_dn, i)]
    fwd_front = [remote(hid.at[2, lo], hid.at[4, lo], h_send.at[4], h_recv.at[4], y_up, i), remote(hid.at[3, hi], hid.at[4, hi], h_send.at[5], h_recv.at[8], y_dn, i)]
    fwd_back = [remote(hid.at[5, lo], hid.at[7, lo], h_send.at[6], h_recv.at[7], y_up, i), remote(hid.at[6, hi], hid.at[7, hi], h_send.at[7], h_recv.at[9], y_dn, i)]

    def chunk_index(p, src_i):
        rank = lax.rem(y + lut(p, PIECE_DY) + n_outer, n_outer) * n_inner + src_i
        return jnp.where(lut(p, PIECE_HALF) == 0, rank, n_chunks - 1 - rank)

    def forward_relay(p, t):
        for c2 in range(2):
            src_x, dst_x = (x_dn, x_up) if c2 == 0 else (x_up, x_dn)
            wait_bytes(relay.at[p, t, c2], r_recv.at[p, t, c2])
            remote(relay.at[p, t, c2], qkv.at[chunk_index(p, src_x * 2 + c), t], r_send, q_recv.at[p], y, dst_x * 2 + c2).start()

    def finish_heads(acc, p, t, j0):
        for u in range(acc.shape[1] // head_dim):
            a = acc[:, u * head_dim:(u + 1) * head_dim]
            if t < 2:
                stage[p, t, j0 + u] = (a * cos_ref[p] + pltpu.roll(a, head_dim // 2, 1) * sin_ref[p]).astype(BF16)
            else:
                stage[p, t, j0 + u] = a.T.astype(BF16)

    def send_piece(p, t):
        out_t = chunk_index(p, i)
        for c2 in range(2):
            via = x_up if c2 == 0 else x_dn
            remote(stage.at[p, t, x_far * 2 + c2], relay.at[p, t, c2], s_send, r_recv.at[p, t, c2], y, via * 2 + c).start()
        for xc in (x_up, x_dn):
            for c2 in range(2):
                remote(stage.at[p, t, xc * 2 + c2], qkv.at[out_t, t], s_send, q_recv.at[p], y, xc * 2 + c2).start()
        other = x * 2 + 1 - c
        remote(stage.at[p, t, other], qkv.at[out_t, t], s_send, q_recv.at[p], y, other).start()
        qkv[out_t, t] = stage[p, t, i]

    n_split = 2
    cols = group // n_split
    per_split = cols // head_dim

    for t in range(3):
        def relayout(k, _, t=t):
            slot = lax.rem(t * n_k + k, n_raw)
            w_copy(t, k, slot).wait()
            wide[...] = raw[slot].astype(F32).reshape(wide.shape)
            for j in range(n_inner):
                big[t, pl.ds(pl.multiple_of(k * depth, depth), depth), j * head_dim:(j + 1) * head_dim] = wide[pl.ds(j, depth, n_inner), :].astype(BF16)
            nxt = k + n_raw

            @pl.when(nxt < n_k)
            def _():
                w_copy(t, nxt, slot).start()

            if t < 2:
                @pl.when(nxt >= n_k)
                def _():
                    w_copy(t + 1, nxt - n_k, slot).start()
            return 0

        k0 = 0
        if t == 0:
            k0 = n_k // 2
            lax.fori_loop(0, k0, relayout, 0)
            with jax.named_scope('barrier'):
                pl.semaphore_wait(barrier, n_dev - 1)
            for cp in send_front:
                cp.start()
        with jax.named_scope(f'relayout{t}'):
            lax.fori_loop(k0, n_k, relayout, 0)
        if t == 0:
            for cp in own:
                cp.wait()
        else:
            for p in range(2):
                with jax.named_scope(f'ownrelay{t}'):
                    forward_relay(p, t - 1)
        def own_rows(n, _, t=t):
            w = big[t, :, pl.ds(pl.multiple_of(n * cols, cols), cols)]
            acc = jnp.dot(hid[0:2].reshape(2 * chunk, model_dim), w, preferred_element_type=F32)
            for p in range(2):
                finish_heads(acc[p * chunk:(p + 1) * chunk], p, t, n * per_split)
            return 0

        with jax.named_scope(f'own{t}'):
            lax.fori_loop(0, n_split, own_rows, 0)
        for p in range(2):
            send_piece(p, t)

    with jax.named_scope('hid23'):
        wait_bytes(hid.at[2], h_recv.at[2])
        wait_bytes(hid.at[3], h_recv.at[3])
    for cp in fwd_front + send_back:
        cp.start()

    def project(p):
        for t in range(3):
            for n in range(n_split):
                acc = jnp.dot(hid[p], big[t, :, n * cols:(n + 1) * cols], preferred_element_type=F32)
                finish_heads(acc, p, t, n * per_split)
            send_piece(p, t)

            @pl.when(jnp.logical_and(p != 2, p != 5))
            def _(t=t):
                forward_relay(p - 1, t)

    def k_tile(j, rows):
        return qkv[pl.ds(j * kc, rows // chunk), 1].reshape(rows, head_dim)

    def vt_tile(j, rows):
        return jnp.concatenate([qkv[j * kc + u, 2] for u in range(rows // chunk)], axis=1)

    def q_strip(b, st):
        n = strip // chunk
        return qkv[pl.ds(b * qc + st * n, n), 0].reshape(strip, head_dim)

    def scores(dst, mx, b, j, st, rows=tk, mask_off=None):
        sl = slice(st * strip, (st + 1) * strip)
        s = lax.dot_general(k_tile(j, rows), q_strip(b, st), (((1,), (1,)), ((), ())), preferred_element_type=F32)
        if mask_off is not None:
            r = lax.broadcasted_iota(jnp.int32, (rows, strip), 0)
            q = lax.broadcasted_iota(jnp.int32, (rows, strip), 1)
            s = jnp.where(r <= q + mask_off, s, NEG_BIG)
        dst[0:rows, sl] = s
        mx[:, sl] = jnp.max(s, axis=0, keepdims=True)

    def update(src, mx, sidx, j, st, rows=tk):
        sl = slice(st * strip, (st + 1) * strip)
        m_old = m_ref[sidx, :, sl]
        m_new = jnp.maximum(m_old, mx[:, sl])
        alpha = jnp.exp2((m_old - m_new) * c_exp)
        p = jnp.exp2((src[0:rows, sl] - m_new) * c_exp)
        l_ref[sidx, :, sl] = l_ref[sidx, :, sl] * alpha + jnp.sum(p, axis=0, keepdims=True)
        m_ref[sidx, :, sl] = m_new
        acc_ref[sidx, :, sl] = acc_ref[sidx, :, sl] * alpha + jnp.dot(vt_tile(j, rows), p.astype(BF16), preferred_element_type=F32)

    def attend(b, sidx, n_kv, key_block, init, diag, finish):
        @pl.when(init)
        def _():
            m_ref[sidx] = jnp.full(m_ref.shape[1:], NEG_BIG, F32)
            l_ref[sidx] = jnp.zeros(l_ref.shape[1:], F32)
            acc_ref[sidx] = jnp.zeros(acc_ref.shape[1:], F32)

        def diag_scores(dst, mx, which, st):
            d = st - which * half
            if 0 <= d < half:
                scores(dst, mx, b, 2 * b + which, st, (d + 1) * strip, d * strip)
            elif d >= half:
                scores(dst, mx, b, 2 * b + which, st)

        def diag_update(src, mx, which, st):
            d = st - which * half
            if d >= 0:
                update(src, mx, sidx, 2 * b + which, st, min(d + 1, half) * strip)

        @pl.when(n_kv > 0)
        def _():
            for st in range(n_strips):
                scores(s0, x0, b, 2 * key_block(0), st)

            def pair(jj, _):
                kb = key_block(jj)
                nxt = key_block(jj + 1)
                for st in range(n_strips):
                    scores(s1, x1, b, 2 * kb + 1, st)
                    update(s0, x0, sidx, 2 * kb, st)
                for st in range(n_strips):
                    scores(s0, x0, b, 2 * nxt, st)
                    update(s1, x1, sidx, 2 * kb + 1, st)
                return 0

            lax.fori_loop(0, n_kv - 1, pair, 0)
            kb = key_block(n_kv - 1)
            for st in range(n_strips):
                scores(s1, x1, b, 2 * kb + 1, st)
                update(s0, x0, sidx, 2 * kb, st)

            @pl.when(diag)
            def _():
                for st in range(n_strips):
                    diag_scores(s0, x0, 0, st)
                    update(s1, x1, sidx, 2 * kb + 1, st)

            @pl.when(jnp.logical_not(diag))
            def _():
                for st in range(n_strips):
                    update(s1, x1, sidx, 2 * kb + 1, st)

        @pl.when(n_kv == 0)
        def _():
            for st in range(n_strips):
                diag_scores(s0, x0, 0, st)

        @pl.when(diag)
        def _():
            for st in range(n_strips):
                diag_scores(s1, x1, 1, st)
                diag_update(s0, x0, 0, st)
            for st in range(n_strips):
                diag_update(s1, x1, 1, st)

        @pl.when(finish)
        def _():
            inv = 1.0 / l_ref[sidx]
            for u in range(qc):
                sl = slice(u * chunk, (u + 1) * chunk)
                qkv[b * qc + u, 0] = (acc_ref[sidx, :, sl] * inv[:, sl]).T.astype(BF16)

    o_cols = pl.ds(pl.multiple_of(me * head_dim, head_dim), head_dim)

    def send_out(b):
        def one(u, _):
            t = b * qc + u
            is_front = t < n_dev
            owner = jnp.where(is_front, t, 2 * n_dev - 1 - t)
            rows = pl.ds(pl.multiple_of(jnp.where(is_front, 0, chunk), chunk), chunk)

            @pl.when(owner == me)
            def _():
                o_recv[rows, o_cols] = qkv[t, 0]

            @pl.when(owner != me)
            def _():
                remote(qkv.at[t, 0], o_recv.at[rows, o_cols], o_send, o_sem.at[y], owner // n_inner, lax.rem(owner, n_inner)).start()
            return 0

        lax.fori_loop(0, qc, one, 0)

    def out_row(r):
        return lax.rem(y + 1 + r, n_outer)

    def wo_copies():
        res = []
        for r in range(n_outer - 1):
            for n in range(n_outer):
                src = wout.at[pl.ds(pl.multiple_of(out_row(r) * group, group), group), pl.ds(n * group, group)]
                res.append(pltpu.make_async_copy(src, big.at[r, pl.ds(n * group, group)], wo_sem.at[r]))
        for u in range(PIECES):
            src = wout.at[pl.ds(pl.multiple_of(y * group + u * chunk, chunk), chunk)]
            res.append(pltpu.make_async_copy(src, hid.at[u], wo_sem.at[n_outer - 1]))
        return res

    kinds = [k for k, _ in STEPS]
    args = [a for _, a in STEPS]

    def step(n, _):
        kind = lut(n, kinds)
        arg = lut(n, args)
        for m, ps in ARRIVE.items():
            @pl.when(n == m)
            def _(ps=ps):
                with jax.named_scope(f'arrive{ps[0]}'):
                    for p in ps:
                        wait_bytes(qkv.at[pl.ds(0, n_inner - 1)], q_recv.at[p])

        @pl.when(n == STEP[PROJ, 4])
        def _():
            with jax.named_scope('hid4'):
                wait_bytes(hid.at[4, lo], h_recv.at[4])
                wait_bytes(hid.at[4, hi], h_recv.at[8])

        @pl.when(n == STEP[PROJ, 5])
        def _():
            with jax.named_scope('hid56'):
                wait_bytes(hid.at[5], h_recv.at[5])
                wait_bytes(hid.at[6], h_recv.at[6])
            for cp in fwd_back:
                cp.start()

        @pl.when(n == STEP[PROJ, 7])
        def _():
            with jax.named_scope('hid7'):
                wait_bytes(hid.at[7, lo], h_recv.at[7])
                wait_bytes(hid.at[7, hi], h_recv.at[9])

        @pl.when(kind == PROJ)
        def _():
            with jax.named_scope('project'):
                project(arg)

        @pl.when(n == STEP[PROJ, 2])
        def _():
            with jax.named_scope('ownrelay3'):
                for p in range(2):
                    forward_relay(p, 2)

        @pl.when(n == STEP[PROJ, 7])
        def _():
            for cp in fwd_front + fwd_back:
                cp.wait_send()
            for cp in wo_copies():
                cp.start()
        @pl.when(kind != PROJ)
        def _():
            shift = jnp.where(kind == EARLY, 0, jnp.where(kind == RECT, arg, lut(arg, ROW_SHIFT)))
            row = lax.rem(y + shift + n_outer, n_outer)
            b = jnp.where(kind == FRONT, row, n_q - 1 - row)
            own_last = jnp.logical_and(kind == LAST, row == y)
            n_early = jnp.where(arg == 0, 1, 2)
            n_last = n_outer - 1 - row + jnp.where(own_last, 1, 0)
            n_kv = jnp.where(kind == EARLY, n_early, jnp.where(kind == FRONT, row, jnp.where(kind == RECT, n_outer, n_last)))

            def key_block(jj):
                early = jnp.where(arg == 0, y, jnp.where(jj == 0, y_dn, y_up))
                last = jnp.where(own_last, jnp.where(jj == 0, lax.rem(y + 2, n_outer), n_outer - 1 + jj), n_outer + jj)
                return jnp.where(kind == EARLY, early, jnp.where(kind == LAST, last, jj))

            sidx = jnp.where(kind == FRONT, n_outer, row)
            finish = jnp.logical_or(kind == FRONT, kind == LAST)
            init = jnp.logical_and(kind != LAST, jnp.logical_not(jnp.logical_and(kind == EARLY, arg == 1)))
            diag = jnp.logical_or(jnp.logical_and(finish, jnp.logical_not(own_last)), jnp.logical_and(kind == EARLY, arg == 0))
            with jax.named_scope('attend'):
                attend(b, sidx, n_kv, key_block, init, diag, finish)

            @pl.when(kind == LAST)
            def _():
                send_out(b)

        for m, ps in FORWARD.items():
            @pl.when(n == m)
            def _(ps=ps):
                with jax.named_scope(f'forward{ps[0]}'):
                    for p in ps:
                        for t in range(3):
                            forward_relay(p, t)

        @pl.when(n == STEP[FRONT, 3])
        def _():
            lax.fori_loop(0, n_outer, lambda k, _: (send_out(lax.rem(y + lut(k, ROW_SHIFT) + n_outer, n_outer)), 0)[1], 0)
        return 0

    lax.fori_loop(0, len(STEPS), step, 0)

    def o_part(r):
        return o_recv[:, pl.ds(pl.multiple_of(out_row(r) * group, group), group)]

    rows = o_recv.shape[0]
    per_buf = tk // rows

    def out_cols(n):
        return pl.ds(pl.multiple_of(n * group, group), group)

    with jax.named_scope('owait0'):
        wait_bytes(qkv.at[pl.ds(0, 2 * n_inner), 0], o_sem.at[out_row(0)])
        wait_bytes(big.at[0], wo_sem.at[0])
    for k, buf in enumerate((s0, s1)):
        def first_part(m, _, k=k, buf=buf):
            buf[pl.ds(pl.multiple_of(m * rows, rows), rows)] = jnp.dot(o_part(0), big[0, out_cols(k * per_buf + m)], preferred_element_type=F32)
            return 0

        with jax.named_scope(f'oproj{k}'):
            lax.fori_loop(0, per_buf, first_part, 0)
    with jax.named_scope('owait1'):
        for r in range(1, n_outer - 1):
            wait_bytes(qkv.at[pl.ds(0, 2 * n_inner), 0], o_sem.at[out_row(r)])
            wait_bytes(big.at[r], wo_sem.at[r])
    with jax.named_scope('owaitown'):
        wait_bytes(qkv.at[pl.ds(0, 2 * (n_inner - 1)), 0], o_sem.at[y])
    wait_bytes(hid, wo_sem.at[n_outer - 1])
    for k, buf in enumerate((s0, s1)):
        def other_parts(m, _, k=k, buf=buf):
            n = k * per_buf + m
            w = hid[:, :, out_cols(n)].reshape(group, group)
            acc = jnp.dot(o_part(n_outer - 1), w, preferred_element_type=F32)
            for r in range(1, n_outer - 1):
                acc = acc + jnp.dot(o_part(r), big[r, out_cols(n)], preferred_element_type=F32)
            out_ref[:, out_cols(n)] = (buf[pl.ds(pl.multiple_of(m * rows, rows), rows)] + acc).astype(BF16)
            return 0

        with jax.named_scope(f'oprojown{k}'):
            lax.fori_loop(0, per_buf, other_parts, 0)

    for cp in send_front + send_back:
        cp.wait_send()
    wait_bytes(stage.at[:, :, pl.ds(0, n_inner - 1)], s_send)
    wait_bytes(relay, r_send)
    wait_bytes(qkv.at[pl.ds(0, 2 * (n_dev - 1)), 0], o_send)


def solution(mesh):
    n_outer = mesh.shape['cpo']
    n_inner = mesh.shape['cpi']
    n_dev = n_outer * n_inner

    def device_step(hidden, w_query, w_key, w_value, w_out):
        rows, model_dim = hidden.shape
        chunk = rows // 2
        n_heads, head_dim = w_query.shape[1:]
        n_chunks = 2 * n_dev
        y = lax.axis_index('cpo')
        i = lax.axis_index('cpi')
        rank = (y + jnp.array(PIECE_DY, jnp.int32)) % n_outer * n_inner + i
        t = jnp.where(jnp.array(PIECE_HALF, jnp.int32) == 0, rank, n_chunks - 1 - rank)
        pos = t[:, None] * chunk + jnp.arange(chunk, dtype=jnp.int32)
        half_dim = head_dim // 2
        lane = jnp.arange(head_dim, dtype=jnp.int32)
        inv_freq = ROPE_BASE ** (-(2.0 / head_dim) * (lane % half_dim).astype(F32))
        angles = pos.astype(F32)[..., None] * inv_freq
        cos_t = jnp.cos(angles)
        sin_t = jnp.sin(angles) * jnp.where(lane < half_dim, -1.0, 1.0)

        any_spec = pl.BlockSpec(memory_space=pl.ANY)
        vmem_spec = pl.BlockSpec(memory_space=pltpu.VMEM)
        dma = pltpu.SemaphoreType.DMA
        depth = 256
        tk, tq = 512, n_inner * chunk
        group = n_inner * head_dim
        return pl.pallas_call(
            functools.partial(layer_kernel, n_outer, n_inner, head_dim ** -0.5),
            out_shape=pltpu.VMEM((rows, model_dim), BF16),
            in_specs=[any_spec] * 5 + [vmem_spec] * 2,
            out_specs=vmem_spec,
            scratch_shapes=[
                pltpu.VMEM((PIECES, chunk, model_dim), BF16),
                pltpu.VMEM((4, depth, n_inner, head_dim), BF16),
                pltpu.VMEM((depth * n_inner, head_dim), F32),
                pltpu.VMEM((3, model_dim, group), BF16),
                pltpu.VMEM((PIECES, 3, n_inner, chunk, head_dim), BF16),
                pltpu.VMEM((PIECES, 3, 2, chunk, head_dim), BF16),
                pltpu.VMEM((n_chunks, 3, chunk, head_dim), BF16),
                pltpu.VMEM((tk, tq), F32),
                pltpu.VMEM((tk, tq), F32),
                pltpu.VMEM((1, tq), F32),
                pltpu.VMEM((1, tq), F32),
                pltpu.VMEM((n_outer + 1, 1, tq), F32),
                pltpu.VMEM((n_outer + 1, 1, tq), F32),
                pltpu.VMEM((n_outer + 1, head_dim, tq), F32),
                pltpu.VMEM((rows, n_heads * head_dim), BF16),
                dma((8,)), dma((10,)), dma((2,)), dma((4,)), dma, dma, dma((PIECES, 3, 2)), dma((PIECES,)), dma((n_outer,)), dma, dma((n_outer,)),
            ],
            compiler_params=pltpu.CompilerParams(collective_id=0, has_side_effects=True, vmem_limit_bytes=60 * 2**20),
            name='layer',
        )(hidden, w_query, w_key, w_value, w_out.reshape(n_heads * head_dim, model_dim), cos_t, sin_t)

    row_spec = P(('dp', 'cpo', 'cpi'), None)
    weight_spec = P(None, None, None)
    return jax.shard_map(device_step, mesh=mesh, in_specs=(row_spec, weight_spec, weight_spec, weight_spec, weight_spec), out_specs=row_spec, check_vma=False)
```

```python
import functools
import math

import jax
import jax.numpy as jnp
from jax import lax
from jax.experimental import pallas as pl
from jax.experimental.pallas import tpu as pltpu
from jax.sharding import PartitionSpec as P

ROPE_BASE = 500000.0
NEG_BIG = -1e30
MESH = pl.DeviceIdType.MESH
F32 = jnp.float32
BF16 = jnp.bfloat16

PIECES = 8
PIECE_HALF = (0, 1, 0, 0, 0, 1, 1, 1)
PIECE_DY = (0, 0, -1, 1, 2, -1, 1, 2)

PROJ, FRONT, RECT, LAST = range(4)
STEPS = (
    (PROJ, 2), (PROJ, 3), (PROJ, 4), (FRONT, 0), (FRONT, 1), (FRONT, 2), (FRONT, 3), (PROJ, 5), (PROJ, 6), (RECT, 0), (PROJ, 7),
    (RECT, -1), (RECT, 1), (RECT, 2), (LAST, 0), (LAST, 1), (LAST, 2), (LAST, 3),
)
STEP = {s: n for n, s in enumerate(STEPS)}
ROW_SHIFT = (2, 1, -1, 0)
FORWARD = {STEP[PROJ, 4]: (4,), STEP[FRONT, 1]: (1,), STEP[RECT, -1]: (7,)}
ARRIVE = {STEP[FRONT, 0]: (0, 2, 3, 4), STEP[RECT, 0]: (1,), STEP[RECT, -1]: (5,), STEP[RECT, 1]: (6,), STEP[RECT, 2]: (7,)}


def lut(n, values):
    out = jnp.int32(values[-1])
    for k in range(len(values) - 2, -1, -1):
        if values[k] != values[k + 1] or k < len(values) - 2:
            out = jnp.where(n == k, jnp.int32(values[k]), out)
    return out


def remote(src, dst, send_sem, recv_sem, y, i):
    return pltpu.make_async_remote_copy(src_ref=src, dst_ref=dst, send_sem=send_sem, recv_sem=recv_sem, device_id={'cpo': y, 'cpi': i}, device_id_type=MESH)


def wait_bytes(ref, sem):
    pltpu.make_async_copy(ref, ref, sem).wait()


def layer_kernel(n_outer, n_inner, score_scale, hid_in, wq, wk, wv, wout, cos_ref, sin_ref, out_ref,
                 hid, raw, wide, big, stage, relay, qkv, s0, s1, x0, x1, m_ref, l_ref, acc_ref, o_recv,
                 h_send, h_recv, h_load, w_sem, s_send, r_send, r_recv, q_recv, wo_sem, o_send, o_sem):
    y = lax.axis_index('cpo')
    i = lax.axis_index('cpi')
    me = y * n_inner + i
    n_dev = n_outer * n_inner
    n_x = n_inner // 2
    x = i // 2
    c = lax.rem(i, 2)
    chunk, model_dim = hid.shape[1:]
    half_rows = chunk // 2
    head_dim = qkv.shape[2]
    n_chunks = qkv.shape[0]
    group = big.shape[2]
    depth = raw.shape[1]
    n_k = model_dim // depth
    n_raw = raw.shape[0]
    y_up = lax.rem(y + 1, n_outer)
    y_dn = lax.rem(y + n_outer - 1, n_outer)
    x_up = lax.rem(x + 1, n_x)
    x_dn = lax.rem(x + n_x - 1, n_x)
    x_far = lax.rem(x + 2, n_x)
    weights = (wq, wk, wv)
    tk, tq = s0.shape
    kc = tk // chunk
    qc = tq // chunk
    n_q = n_chunks // qc
    strip = 256
    n_strips = tq // strip
    half = n_strips // 2
    c_exp = score_scale * math.log2(math.e)

    def w_copy(t, k, slot):
        src = weights[t].at[pl.ds(k * depth, depth), pl.ds(pl.multiple_of(y * n_inner, n_inner), n_inner)]
        return pltpu.make_async_copy(src, raw.at[slot], w_sem.at[slot])

    for slot in range(n_raw):
        w_copy(0, slot, slot).start()
    own = [pltpu.make_async_copy(hid_in.at[pl.ds(f * chunk, chunk)], hid.at[f], h_load.at[f]) for f in range(2)]
    for cp in own:
        cp.start()

    barrier = pltpu.get_barrier_semaphore()

    def sig(d, _):
        peer = lax.rem(me + d, n_dev)
        pl.semaphore_signal(barrier, inc=1, device_id={'cpo': peer // n_inner, 'cpi': lax.rem(peer, n_inner)}, device_id_type=MESH)
        return 0

    lax.fori_loop(1, n_dev, sig, 0)

    front = hid_in.at[pl.ds(0, chunk)]
    back = hid_in.at[pl.ds(chunk, chunk)]
    lo, hi = pl.ds(0, half_rows), pl.ds(half_rows, half_rows)
    send_front = [remote(front, hid.at[2], h_send.at[0], h_recv.at[2], y_up, i), remote(front, hid.at[3], h_send.at[1], h_recv.at[3], y_dn, i)]
    send_back = [remote(back, hid.at[5], h_send.at[2], h_recv.at[5], y_up, i), remote(back, hid.at[6], h_send.at[3], h_recv.at[6], y_dn, i)]
    fwd_front = [remote(hid.at[2, lo], hid.at[4, lo], h_send.at[4], h_recv.at[4], y_up, i), remote(hid.at[3, hi], hid.at[4, hi], h_send.at[5], h_recv.at[8], y_dn, i)]
    fwd_back = [remote(hid.at[5, lo], hid.at[7, lo], h_send.at[6], h_recv.at[7], y_up, i), remote(hid.at[6, hi], hid.at[7, hi], h_send.at[7], h_recv.at[9], y_dn, i)]

    def chunk_index(p, src_i):
        rank = lax.rem(y + lut(p, PIECE_DY) + n_outer, n_outer) * n_inner + src_i
        return jnp.where(lut(p, PIECE_HALF) == 0, rank, n_chunks - 1 - rank)

    def forward_relay(p, t):
        for c2 in range(2):
            src_x, dst_x = (x_dn, x_up) if c2 == 0 else (x_up, x_dn)
            wait_bytes(relay.at[p, t, c2], r_recv.at[p, t, c2])
            remote(relay.at[p, t, c2], qkv.at[chunk_index(p, src_x * 2 + c), t], r_send, q_recv.at[p], y, dst_x * 2 + c2).start()

    def finish_heads(acc, p, t, j0):
        for u in range(acc.shape[1] // head_dim):
            a = acc[:, u * head_dim:(u + 1) * head_dim]
            if t < 2:
                stage[p, t, j0 + u] = (a * cos_ref[p] + pltpu.roll(a, head_dim // 2, 1) * sin_ref[p]).astype(BF16)
            else:
                stage[p, t, j0 + u] = a.T.astype(BF16)

    def send_piece(p, t):
        out_t = chunk_index(p, i)
        for c2 in range(2):
            via = x_up if c2 == 0 else x_dn
            remote(stage.at[p, t, x_far * 2 + c2], relay.at[p, t, c2], s_send, r_recv.at[p, t, c2], y, via * 2 + c).start()
        for xc in (x_up, x_dn):
            for c2 in range(2):
                remote(stage.at[p, t, xc * 2 + c2], qkv.at[out_t, t], s_send, q_recv.at[p], y, xc * 2 + c2).start()
        other = x * 2 + 1 - c
        remote(stage.at[p, t, other], qkv.at[out_t, t], s_send, q_recv.at[p], y, other).start()
        qkv[out_t, t] = stage[p, t, i]

    n_split = 2
    cols = group // n_split
    per_split = cols // head_dim

    for t in range(3):
        def relayout(k, _, t=t):
            slot = lax.rem(t * n_k + k, n_raw)
            w_copy(t, k, slot).wait()
            wide[...] = raw[slot].astype(F32).reshape(wide.shape)
            for j in range(n_inner):
                big[t, pl.ds(pl.multiple_of(k * depth, depth), depth), j * head_dim:(j + 1) * head_dim] = wide[pl.ds(j, depth, n_inner), :].astype(BF16)
            nxt = k + n_raw

            @pl.when(nxt < n_k)
            def _():
                w_copy(t, nxt, slot).start()

            if t < 2:
                @pl.when(nxt >= n_k)
                def _():
                    w_copy(t + 1, nxt - n_k, slot).start()
            return 0

        k0 = 0
        if t == 0:
            k0 = n_k // 2
            lax.fori_loop(0, k0, relayout, 0)
            with jax.named_scope('barrier'):
                pl.semaphore_wait(barrier, n_dev - 1)
            for cp in send_front:
                cp.start()
        with jax.named_scope(f'relayout{t}'):
            lax.fori_loop(k0, n_k, relayout, 0)
        if t == 0:
            for cp in own:
                cp.wait()
        else:
            with jax.named_scope(f'ownrelay{t}'):
                forward_relay(0, t - 1)
        def own_rows(n, _, t=t):
            w = big[t, :, pl.ds(pl.multiple_of(n * cols, cols), cols)]
            acc = jnp.dot(hid[0:2].reshape(2 * chunk, model_dim), w, preferred_element_type=F32)
            for p in range(2):
                finish_heads(acc[p * chunk:(p + 1) * chunk], p, t, n * per_split)
            return 0

        with jax.named_scope(f'own{t}'):
            lax.fori_loop(0, n_split, own_rows, 0)
        send_piece(0, t)

    with jax.named_scope('hid23'):
        wait_bytes(hid.at[2], h_recv.at[2])
        wait_bytes(hid.at[3], h_recv.at[3])
    for cp in fwd_front + send_back:
        cp.start()

    def project(p):
        for t in range(3):
            for n in range(n_split):
                acc = jnp.dot(hid[p], big[t, :, n * cols:(n + 1) * cols], preferred_element_type=F32)
                finish_heads(acc, p, t, n * per_split)
            send_piece(p, t)

            @pl.when(jnp.logical_and(p != 2, p != 5))
            def _(t=t):
                forward_relay(p - 1, t)

    def k_tile(j, rows):
        return qkv[pl.ds(j * kc, rows // chunk), 1].reshape(rows, head_dim)

    def vt_tile(j, rows):
        return jnp.concatenate([qkv[j * kc + u, 2] for u in range(rows // chunk)], axis=1)

    def q_strip(b, st):
        n = strip // chunk
        return qkv[pl.ds(b * qc + st * n, n), 0].reshape(strip, head_dim)

    def scores(dst, mx, b, j, st, rows=tk, mask_off=None):
        sl = slice(st * strip, (st + 1) * strip)
        s = lax.dot_general(k_tile(j, rows), q_strip(b, st), (((1,), (1,)), ((), ())), preferred_element_type=F32)
        if mask_off is not None:
            r = lax.broadcasted_iota(jnp.int32, (rows, strip), 0)
            q = lax.broadcasted_iota(jnp.int32, (rows, strip), 1)
            s = jnp.where(r <= q + mask_off, s, NEG_BIG)
        dst[0:rows, sl] = s
        mx[:, sl] = jnp.max(s, axis=0, keepdims=True)

    def update(src, mx, sidx, j, st, rows=tk):
        sl = slice(st * strip, (st + 1) * strip)
        m_old = m_ref[sidx, :, sl]
        m_new = jnp.maximum(m_old, mx[:, sl])
        alpha = jnp.exp2((m_old - m_new) * c_exp)
        p = jnp.exp2((src[0:rows, sl] - m_new) * c_exp)
        l_ref[sidx, :, sl] = l_ref[sidx, :, sl] * alpha + jnp.sum(p, axis=0, keepdims=True)
        m_ref[sidx, :, sl] = m_new
        acc_ref[sidx, :, sl] = acc_ref[sidx, :, sl] * alpha + jnp.dot(vt_tile(j, rows), p.astype(BF16), preferred_element_type=F32)

    def attend(b, sidx, n_kv, key_block, init, diag, finish):
        @pl.when(init)
        def _():
            m_ref[sidx] = jnp.full(m_ref.shape[1:], NEG_BIG, F32)
            l_ref[sidx] = jnp.zeros(l_ref.shape[1:], F32)
            acc_ref[sidx] = jnp.zeros(acc_ref.shape[1:], F32)

        def diag_scores(dst, mx, which, st):
            d = st - which * half
            if 0 <= d < half:
                scores(dst, mx, b, 2 * b + which, st, (d + 1) * strip, d * strip)
            elif d >= half:
                scores(dst, mx, b, 2 * b + which, st)

        def diag_update(src, mx, which, st):
            d = st - which * half
            if d >= 0:
                update(src, mx, sidx, 2 * b + which, st, min(d + 1, half) * strip)

        @pl.when(n_kv > 0)
        def _():
            for st in range(n_strips):
                scores(s0, x0, b, 2 * key_block(0), st)

            def pair(jj, _):
                kb = key_block(jj)
                nxt = key_block(jj + 1)
                for st in range(n_strips):
                    scores(s1, x1, b, 2 * kb + 1, st)
                    update(s0, x0, sidx, 2 * kb, st)
                for st in range(n_strips):
                    scores(s0, x0, b, 2 * nxt, st)
                    update(s1, x1, sidx, 2 * kb + 1, st)
                return 0

            lax.fori_loop(0, n_kv - 1, pair, 0)
            kb = key_block(n_kv - 1)
            for st in range(n_strips):
                scores(s1, x1, b, 2 * kb + 1, st)
                update(s0, x0, sidx, 2 * kb, st)

            @pl.when(diag)
            def _():
                for st in range(n_strips):
                    diag_scores(s0, x0, 0, st)
                    update(s1, x1, sidx, 2 * kb + 1, st)

            @pl.when(jnp.logical_not(diag))
            def _():
                for st in range(n_strips):
                    update(s1, x1, sidx, 2 * kb + 1, st)

        @pl.when(n_kv == 0)
        def _():
            for st in range(n_strips):
                diag_scores(s0, x0, 0, st)

        @pl.when(diag)
        def _():
            for st in range(n_strips):
                diag_scores(s1, x1, 1, st)
                diag_update(s0, x0, 0, st)
            for st in range(n_strips):
                diag_update(s1, x1, 1, st)

        @pl.when(finish)
        def _():
            inv = 1.0 / l_ref[sidx]
            for u in range(qc):
                sl = slice(u * chunk, (u + 1) * chunk)
                qkv[b * qc + u, 0] = (acc_ref[sidx, :, sl] * inv[:, sl]).T.astype(BF16)

    o_cols = pl.ds(pl.multiple_of(me * head_dim, head_dim), head_dim)

    def send_out(b):
        def one(u, _):
            t = b * qc + u
            is_front = t < n_dev
            owner = jnp.where(is_front, t, 2 * n_dev - 1 - t)
            rows = pl.ds(pl.multiple_of(jnp.where(is_front, 0, chunk), chunk), chunk)

            @pl.when(owner == me)
            def _():
                o_recv[rows, o_cols] = qkv[t, 0]

            @pl.when(owner != me)
            def _():
                remote(qkv.at[t, 0], o_recv.at[rows, o_cols], o_send, o_sem.at[y], owner // n_inner, lax.rem(owner, n_inner)).start()
            return 0

        lax.fori_loop(0, qc, one, 0)

    def out_row(r):
        return lax.rem(y + 1 + r, n_outer)

    def wo_copies():
        res = []
        for r in range(n_outer - 1):
            for n in range(n_outer):
                src = wout.at[pl.ds(pl.multiple_of(out_row(r) * group, group), group), pl.ds(n * group, group)]
                res.append(pltpu.make_async_copy(src, big.at[r, pl.ds(n * group, group)], wo_sem.at[r]))
        for u in range(PIECES):
            src = wout.at[pl.ds(pl.multiple_of(y * group + u * chunk, chunk), chunk)]
            res.append(pltpu.make_async_copy(src, hid.at[u], wo_sem.at[n_outer - 1]))
        return res

    kinds = [k for k, _ in STEPS]
    args = [a for _, a in STEPS]

    def step(n, _):
        kind = lut(n, kinds)
        arg = lut(n, args)
        for m, ps in ARRIVE.items():
            @pl.when(n == m)
            def _(ps=ps):
                with jax.named_scope(f'arrive{ps[0]}'):
                    for p in ps:
                        wait_bytes(qkv.at[pl.ds(0, n_inner - 1)], q_recv.at[p])

        @pl.when(n == STEP[PROJ, 4])
        def _():
            with jax.named_scope('hid4'):
                wait_bytes(hid.at[4, lo], h_recv.at[4])
                wait_bytes(hid.at[4, hi], h_recv.at[8])

        @pl.when(n == STEP[PROJ, 5])
        def _():
            with jax.named_scope('hid56'):
                wait_bytes(hid.at[5], h_recv.at[5])
                wait_bytes(hid.at[6], h_recv.at[6])
            for cp in fwd_back:
                cp.start()

        @pl.when(n == STEP[PROJ, 7])
        def _():
            with jax.named_scope('hid7'):
                wait_bytes(hid.at[7, lo], h_recv.at[7])
                wait_bytes(hid.at[7, hi], h_recv.at[9])
            send_out(lax.rem(y + ROW_SHIFT[0] + n_outer, n_outer))

        @pl.when(kind == PROJ)
        def _():
            with jax.named_scope('project'):
                project(arg)

        @pl.when(n == STEP[PROJ, 2])
        def _():
            with jax.named_scope('ownrelay3'):
                forward_relay(0, 2)

        @pl.when(n == STEP[PROJ, 7])
        def _():
            for cp in fwd_front + fwd_back:
                cp.wait_send()
            for cp in wo_copies():
                cp.start()
        @pl.when(kind != PROJ)
        def _():
            shift = jnp.where(kind == RECT, arg, lut(arg, ROW_SHIFT))
            row = lax.rem(y + shift + n_outer, n_outer)
            b = jnp.where(kind == FRONT, row, n_q - 1 - row)
            n_kv = jnp.where(kind == FRONT, row, jnp.where(kind == RECT, n_outer, n_outer - 1 - row))

            def key_block(jj):
                return jnp.where(kind == LAST, n_outer + jj, jj)

            sidx = jnp.where(kind == FRONT, n_outer, row)
            finish = kind != RECT
            init = kind != LAST
            diag = finish
            with jax.named_scope('attend'):
                attend(b, sidx, n_kv, key_block, init, diag, finish)

            @pl.when(kind == LAST)
            def _():
                send_out(b)

        for m, ps in FORWARD.items():
            @pl.when(n == m)
            def _(ps=ps):
                with jax.named_scope(f'forward{ps[0]}'):
                    for p in ps:
                        for t in range(3):
                            forward_relay(p, t)

        @pl.when(n == STEP[PROJ, 4])
        def _():
            for t in range(3):
                send_piece(1, t)

        @pl.when(n == STEP[RECT, -1])
        def _():
            lax.fori_loop(1, n_outer, lambda k, _: (send_out(lax.rem(y + lut(k, ROW_SHIFT) + n_outer, n_outer)), 0)[1], 0)
        return 0

    lax.fori_loop(0, len(STEPS), step, 0)

    def o_part(r):
        return o_recv[:, pl.ds(pl.multiple_of(out_row(r) * group, group), group)]

    rows = o_recv.shape[0]
    per_buf = tk // rows

    def out_cols(n):
        return pl.ds(pl.multiple_of(n * group, group), group)

    with jax.named_scope('owait0'):
        wait_bytes(qkv.at[pl.ds(0, 2 * n_inner), 0], o_sem.at[out_row(0)])
        wait_bytes(big.at[0], wo_sem.at[0])
    for k, buf in enumerate((s0, s1)):
        def first_part(m, _, k=k, buf=buf):
            buf[pl.ds(pl.multiple_of(m * rows, rows), rows)] = jnp.dot(o_part(0), big[0, out_cols(k * per_buf + m)], preferred_element_type=F32)
            return 0

        with jax.named_scope(f'oproj{k}'):
            lax.fori_loop(0, per_buf, first_part, 0)
    with jax.named_scope('owait1'):
        for r in range(1, n_outer - 1):
            wait_bytes(qkv.at[pl.ds(0, 2 * n_inner), 0], o_sem.at[out_row(r)])
            wait_bytes(big.at[r], wo_sem.at[r])
    with jax.named_scope('owaitown'):
        wait_bytes(qkv.at[pl.ds(0, 2 * (n_inner - 1)), 0], o_sem.at[y])
    wait_bytes(hid, wo_sem.at[n_outer - 1])
    for k, buf in enumerate((s0, s1)):
        def other_parts(m, _, k=k, buf=buf):
            n = k * per_buf + m
            w = hid[:, :, out_cols(n)].reshape(group, group)
            acc = jnp.dot(o_part(n_outer - 1), w, preferred_element_type=F32)
            for r in range(1, n_outer - 1):
                acc = acc + jnp.dot(o_part(r), big[r, out_cols(n)], preferred_element_type=F32)
            out_ref[:, out_cols(n)] = (buf[pl.ds(pl.multiple_of(m * rows, rows), rows)] + acc).astype(BF16)
            return 0

        with jax.named_scope(f'oprojown{k}'):
            lax.fori_loop(0, per_buf, other_parts, 0)

    for cp in send_front + send_back:
        cp.wait_send()
    wait_bytes(stage.at[:, :, pl.ds(0, n_inner - 1)], s_send)
    wait_bytes(relay, r_send)
    wait_bytes(qkv.at[pl.ds(0, 2 * (n_dev - 1)), 0], o_send)


def solution(mesh):
    n_outer = mesh.shape['cpo']
    n_inner = mesh.shape['cpi']
    n_dev = n_outer * n_inner

    def device_step(hidden, w_query, w_key, w_value, w_out):
        rows, model_dim = hidden.shape
        chunk = rows // 2
        n_heads, head_dim = w_query.shape[1:]
        n_chunks = 2 * n_dev
        y = lax.axis_index('cpo')
        i = lax.axis_index('cpi')
        rank = (y + jnp.array(PIECE_DY, jnp.int32)) % n_outer * n_inner + i
        t = jnp.where(jnp.array(PIECE_HALF, jnp.int32) == 0, rank, n_chunks - 1 - rank)
        pos = t[:, None] * chunk + jnp.arange(chunk, dtype=jnp.int32)
        half_dim = head_dim // 2
        lane = jnp.arange(head_dim, dtype=jnp.int32)
        inv_freq = ROPE_BASE ** (-(2.0 / head_dim) * (lane % half_dim).astype(F32))
        angles = pos.astype(F32)[..., None] * inv_freq
        cos_t = jnp.cos(angles)
        sin_t = jnp.sin(angles) * jnp.where(lane < half_dim, -1.0, 1.0)

        any_spec = pl.BlockSpec(memory_space=pl.ANY)
        vmem_spec = pl.BlockSpec(memory_space=pltpu.VMEM)
        dma = pltpu.SemaphoreType.DMA
        depth = 256
        tk, tq = 512, n_inner * chunk
        group = n_inner * head_dim
        return pl.pallas_call(
            functools.partial(layer_kernel, n_outer, n_inner, head_dim ** -0.5),
            out_shape=pltpu.VMEM((rows, model_dim), BF16),
            in_specs=[any_spec] * 5 + [vmem_spec] * 2,
            out_specs=vmem_spec,
            scratch_shapes=[
                pltpu.VMEM((PIECES, chunk, model_dim), BF16),
                pltpu.VMEM((4, depth, n_inner, head_dim), BF16),
                pltpu.VMEM((depth * n_inner, head_dim), F32),
                pltpu.VMEM((3, model_dim, group), BF16),
                pltpu.VMEM((PIECES, 3, n_inner, chunk, head_dim), BF16),
                pltpu.VMEM((PIECES, 3, 2, chunk, head_dim), BF16),
                pltpu.VMEM((n_chunks, 3, chunk, head_dim), BF16),
                pltpu.VMEM((tk, tq), F32),
                pltpu.VMEM((tk, tq), F32),
                pltpu.VMEM((1, tq), F32),
                pltpu.VMEM((1, tq), F32),
                pltpu.VMEM((n_outer + 1, 1, tq), F32),
                pltpu.VMEM((n_outer + 1, 1, tq), F32),
                pltpu.VMEM((n_outer + 1, head_dim, tq), F32),
                pltpu.VMEM((rows, n_heads * head_dim), BF16),
                dma((8,)), dma((10,)), dma((2,)), dma((4,)), dma, dma, dma((PIECES, 3, 2)), dma((PIECES,)), dma((n_outer,)), dma, dma((n_outer,)),
            ],
            compiler_params=pltpu.CompilerParams(collective_id=0, has_side_effects=True, vmem_limit_bytes=60 * 2**20),
            name='layer',
        )(hidden, w_query, w_key, w_value, w_out.reshape(n_heads * head_dim, model_dim), cos_t, sin_t)

    row_spec = P(('dp', 'cpo', 'cpi'), None)
    weight_spec = P(None, None, None)
    return jax.shard_map(device_step, mesh=mesh, in_specs=(row_spec, weight_spec, weight_spec, weight_spec, weight_spec), out_specs=row_spec, check_vma=False)
```
